8 devices in a mesh: rep: 1 (over z), dp: 8 (over x, y, core).
Axes of the slice: x: 2, y: 2, z: 1, core: 2. Of those that a mesh axis runs over, the one named last changes fastest.
Arguments:
- x: bfloat16 [8, 2048, 1024], P(('rep', 'dp'))
- dy: bfloat16 [8, 2048, 1024], P(('rep', 'dp'))
- w_gate: bfloat16 [2, 1024, 2560], P(None, 'dp')
- w_up: bfloat16 [2, 1024, 2560], P(None, 'dp')
- w_down: bfloat16 [2, 2560, 1024], P(None, 'dp')
Outputs:
- output 1: bfloat16 [8, 2048, 1024], P(('rep', 'dp'))
- output 2: bfloat16 [2, 1024, 2560], P('rep', 'dp')
- output 3: bfloat16 [2, 1024, 2560], P('rep', 'dp')
- output 4: bfloat16 [2, 2560, 1024], P('rep', 'dp')
All inputs are finite; a program needn't handle non-finite values.
Results may differ from the reference program's by a relative error of at most 0.018.
Values are sent between devices in bfloat16 or wider.
A program may use at most 2 GiB of HBM per device.

```python
import jax
import jax.numpy as jnp
from jax import lax

SEQUENCES = 8
TOKENS = 2048
D = 1024
FF = 2560
LAYERS = 2
NAMES = ("w_gate", "w_up", "w_down")
SHAPES = {"w_gate": (LAYERS, D, FF), "w_up": (LAYERS, D, FF), "w_down": (LAYERS, FF, D)}


def bump(key, n, height):
    away = (jnp.arange(n, dtype=jnp.int32) - jax.random.randint(key, (), 0, n, jnp.int32)) % n
    return jnp.where(away < n // 8, height, 1.0)


def together(key, own, strength):
    shared = jax.random.normal(key, own.shape[1:], jnp.float32)
    return (own + strength * shared) * lax.rsqrt(1 + strength * strength)


def setup_inputs(seed: int = 0, part: int = 0) -> dict:
    kx, kdy, ka, kb, kz, kf, kh, kl, *kw = jax.random.split(jax.random.key(seed), 8 + len(NAMES))
    kx, kdy, ka, kb = (jax.random.fold_in(k, part) for k in (kx, kdy, ka, kb))
    shape = (SEQUENCES, TOKENS, D)
    much_x, much_dy = jax.random.uniform(kz, (2,), jnp.float32, 0.0, 1.0)
    layers = 2.0 ** jax.random.uniform(kl, (LAYERS, 1, 1), jnp.float32, -1.0, 1.0)
    x = together(ka, jax.random.normal(kx, shape, jnp.float32), much_x) * bump(kf, D, 4.0)
    dy = together(kb, jax.random.normal(kdy, shape, jnp.float32), much_dy)
    drawn = {"x": x.astype(jnp.bfloat16), "dy": (dy * (SEQUENCES * TOKENS) ** -0.5).astype(jnp.bfloat16)}
    for key, name in zip(kw, NAMES, strict=True):
        w = jax.random.normal(key, SHAPES[name], jnp.float32) * SHAPES[name][1] ** -0.5
        drawn[name] = (w * {"w_gate": 1.0, "w_up": bump(kh, FF, 4.0), "w_down": layers}[name]).astype(jnp.bfloat16)
    return drawn


def matmul(a, w):
    return jnp.dot(a, w, preferred_element_type=jnp.float32).astype(jnp.bfloat16)


def normed(h):
    wide = h.astype(jnp.float32)
    scale = lax.rsqrt(jnp.mean(wide**2, -1, keepdims=True) + 1e-6)
    return (wide * scale).astype(jnp.bfloat16)


def layer(h, w):
    a = normed(h)
    gate = jnp.dot(a, w["w_gate"], preferred_element_type=jnp.float32)
    up = jnp.dot(a, w["w_up"], preferred_element_type=jnp.float32)
    return h + matmul((jax.nn.silu(gate) * up).astype(jnp.bfloat16), w["w_down"])


def stack(weights, h):
    return lax.scan(lambda h, w: (layer(h, w), None), h, weights)[0]


def reference(x, dy, w_gate, w_up, w_down):
    weights = dict(zip(NAMES, (w_gate, w_up, w_down), strict=True))

    def take(so_far, sequence):
        h, by_y = sequence
        _, back = jax.vjp(stack, weights, h)
        by_weights, by_h = back(by_y)
        return jax.tree.map(lambda total, term: total + term.astype(jnp.float32), so_far, by_weights), by_h

    none_yet = {name: jnp.zeros(w.shape, jnp.float32) for name, w in weights.items()}
    by_weights, by_x = lax.scan(take, none_yet, (x, dy))
    return (by_x, *(by_weights[name].astype(jnp.bfloat16) for name in NAMES))
```

```python
import jax
import jax.numpy as jnp
from jax import lax
from jax.sharding import PartitionSpec as P

F32, BF16 = jnp.float32, jnp.bfloat16


def dot(a, b, dims):
    return lax.dot_general(a, b, (dims, ((), ())), preferred_element_type=F32)


def norm(h):
    wide = h.astype(F32)
    scale = lax.rsqrt(jnp.mean(wide**2, -1, keepdims=True) + 1e-6)
    return wide, scale, (wide * scale).astype(BF16)


def solution(mesh):
    def gather(w):
        return lax.all_gather(w, "dp", axis=0, tiled=True)

    def scatter(g):
        return lax.psum_scatter(g.astype(BF16), "dp", scatter_dimension=0, tiled=True)

    def body(x, dy, wg, wu, wd):
        layers = wg.shape[0]
        h, dh = x[0], dy[0]
        weights = [tuple(gather(w[n]) for w in (wg, wu, wd)) for n in range(layers)]
        saved = []
        for n in range(layers):
            g_w, u_w, d_w = weights[n]
            wide, scale, a = norm(h)
            gate = dot(a, g_w, ((1,), (0,)))
            up = dot(a, u_w, ((1,), (0,)))
            p = (jax.nn.silu(gate) * up).astype(BF16)
            saved.append((wide, scale, a, gate, up, p))
            if n + 1 < layers:
                h = h + dot(p, d_w, ((1,), (0,))).astype(BF16)
        grads = [None] * layers
        for n in reversed(range(layers)):
            g_w, u_w, d_w = weights[n]
            wide, scale, a, gate, up, p = saved[n]
            dp = dot(dh, d_w, ((1,), (1,))).astype(BF16).astype(F32)
            by_d = scatter(dot(p, dh, ((0,), (0,))))
            sig = jax.nn.sigmoid(gate)
            d_gate = (dp * up * (sig * (1 + gate * (1 - sig)))).astype(BF16)
            d_up = (dp * (gate * sig)).astype(BF16)
            by_g = scatter(dot(a, d_gate, ((0,), (0,))))
            by_u = scatter(dot(a, d_up, ((0,), (0,))))
            da = dot(d_gate, g_w, ((1,), (1,))) + dot(d_up, u_w, ((1,), (1,)))
            da = da.astype(BF16).astype(F32)
            inner = jnp.mean(da * wide, -1, keepdims=True)
            back = scale * da - wide * (scale**3 * inner)
            dh = dh + back.astype(BF16)
            grads[n] = (by_g, by_u, by_d)
        return (dh[None], *(jnp.stack([g[i] for g in grads]) for i in range(3)))

    act = P(("rep", "dp"), None, None)
    w = P(None, "dp", None)
    return jax.shard_map(
        body, mesh=mesh, in_specs=(act, act, w, w, w), out_specs=(act, *[P("rep", "dp", None)] * 3), check_vma=False
    )
```

```python
import functools

import jax
import jax.numpy as jnp
from jax import lax
from jax.experimental import pallas as pl
from jax.experimental.pallas import tpu as pltpu
from jax.sharding import PartitionSpec as P

F32, BF16 = jnp.float32, jnp.bfloat16
T, D, FF, L, N = 2048, 1024, 2560, 2, 8
NC = 5
HC = FF // NC
SEG = HC // N
RD = D // N
K = L * NC
TT = 512
NT = T // TT
TE = 256
NN = (((1,), (0,)), ((), ()))
NT_DIMS = (((1,), (1,)), ((), ()))


def dot(a, b):
    return lax.dot_general(a, b, NN, preferred_element_type=F32)


def dot_nt(a, b):
    return lax.dot_general(a, b, NT_DIMS, preferred_element_type=F32)


def kernel(
    x_hbm, dy_hbm, own,
    dx_hbm, out, land,
    xh, a_ref, at_ref, dh, acc, wgu, wdn, pt, dg, du,
    keep, send0, recv0, s1, r1, s2, r2, outb,
    ag_send, ag_recv, rs_send, rs_recv, gu_sem, wd_sem, io_sem, out_sem,
):
    me = lax.axis_index("dp")
    core = me % 2
    ypos = (me // 2) % 2
    xpos = me // 4
    xn = (1 - xpos) * 4 + ypos * 2 + core
    yn = xpos * 4 + (1 - ypos) * 2 + core
    cn = xpos * 4 + ypos * 2 + (1 - core)
    diag = (1 - xpos) * 4 + (1 - ypos) * 2 + core
    q_me, q_x, q_y, q_d = me // 2, xn // 2, yn // 2, diag // 2

    def remote(src, dst, ssem, rsem, dev):
        return pltpu.make_async_remote_copy(
            src_ref=src, dst_ref=dst, send_sem=ssem, recv_sem=rsem,
            device_id={"dp": dev}, device_id_type=pl.DeviceIdType.MESH,
        )

    LO, HI = pl.ds(0, RD // 2), pl.ds(RD // 2, RD // 2)

    def ag(k, m, arriving=False):
        if m < 3:
            dev, src, dst, got = (xn, yn, cn)[m], own.at[k], land.at[k, me], land.at[k, (xn, yn, cn)[m]]
        elif m == 3:
            dev, src, dst, got = yn, land.at[k, xn, :, LO], land.at[k, xn, :, LO], land.at[k, diag, :, LO]
        elif m == 4:
            dev, src, dst, got = xn, land.at[k, yn, :, HI], land.at[k, yn, :, HI], land.at[k, diag, :, HI]
        else:
            b = (xn, yn, diag)[m - 5]
            there = (b // 2) * 2 + (1 - core)
            dev, src, dst, got = cn, land.at[k, b], land.at[k, b], land.at[k, there]
        if arriving:
            src = dst = got
        return remote(src, dst, ag_send.at[k, m], ag_recv.at[k, m], dev)

    def ag_start(k, ms):
        for m in ms:
            ag(k, m).start()

    def ag_wait(k, ms):
        for m in ms:
            ag(k, m, True).wait_recv()

    def load(p):
        k, slot = p % K, p % 2
        for r in range(N):
            if r == 0:
                j, src = me, own.at[k]
            else:
                fx, fy, fc = r // 4, (r // 2) % 2, r % 2
                j = ((xpos + fx) % 2) * 4 + ((ypos + fy) % 2) * 2 + (core + fc) % 2
                src = land.at[k, j]
            rows, segs = pl.ds(j * RD, RD), pl.ds(j * SEG, SEG)
            pltpu.make_async_copy(src.at[pl.ds(0, 2)], wgu.at[slot, :, rows, :], gu_sem.at[slot]).start()
            for h in range(2):
                pltpu.make_async_copy(
                    src.at[2, pl.ds(h * SEG, SEG)], wdn.at[slot, segs, pl.ds(h * HC, HC)], wd_sem.at[slot]
                ).start()

    def load_wait(p):
        slot = p % 2
        pltpu.make_async_copy(wgu.at[slot], wgu.at[slot], gu_sem.at[slot]).wait()
        pltpu.make_async_copy(wdn.at[slot], wdn.at[slot], wd_sem.at[slot]).wait()

    def tick(t):
        @pl.when(t < K)
        def _():
            ag_wait(t, (0, 1))
            ag_start(t, (3, 4, 5, 6))

        @pl.when(t + 2 < K)
        def _():
            ag_start(t + 2, (0, 1, 2))

        @pl.when((t >= 1) & (t - 1 < K))
        def _():
            ag_wait(t - 1, (3, 4))
            ag_start(t - 1, (7,))
            ag_wait(t - 1, (2, 5, 6, 7))

        @pl.when((t >= 1) & (t - 1 < K + NC))
        def _():
            load(t - 1)

    def rs(v, m):
        src, dst, dev = (
            (send0, recv0.at[v], cn),
            (s1.at[0], r1.at[v, 0], xn),
            (s1.at[1], r1.at[v, 1], yn),
            (s2.at[0], r2.at[v, 0], xn),
            (s2.at[1], r2.at[v, 1], yn),
        )[m]
        return remote(src, dst, rs_send.at[m], rs_recv.at[v, m], dev)

    def half(q, h):
        return pl.ds(q * RD + h * (RD // 2), RD // 2)

    def block(q):
        return pl.ds(q * RD, RD)

    def f1(b):
        v = b % 2
        rs(v, 0).wait_recv()

        @pl.when(b >= 1)
        def _():
            rs(v, 1).wait_send()
            rs(v, 2).wait_send()

        for i in range(3):
            keep[v, i] = keep[v, i] + recv0[v, i].astype(F32)
        for i in range(3):
            s1[0, i] = keep[v, i, half(q_d, 0), :].astype(BF16)
            s1[1, i] = keep[v, i, half(q_d, 1), :].astype(BF16)
        rs(v, 1).start()
        rs(v, 2).start()

    def f2(b):
        v = b % 2
        rs(v, 1).wait_recv()
        rs(v, 2).wait_recv()

        @pl.when(b >= 1)
        def _():
            rs(v, 3).wait_send()
            rs(v, 4).wait_send()

        for i in range(3):
            keep[v, i, half(q_y, 0), :] = keep[v, i, half(q_y, 0), :] + r1[v, 0, i].astype(F32)
            keep[v, i, half(q_x, 1), :] = keep[v, i, half(q_x, 1), :] + r1[v, 1, i].astype(F32)
        for i in range(3):
            s2[0, i] = keep[v, i, block(q_x), :].astype(BF16)
            s2[1, i] = keep[v, i, block(q_y), :].astype(BF16)
        rs(v, 3).start()
        rs(v, 4).start()

    def out_copy(b):
        return pltpu.make_async_copy(outb, out.at[(b + NC) % K], out_sem)

    def f3(b):
        v = b % 2
        rs(v, 3).wait_recv()
        rs(v, 4).wait_recv()

        @pl.when(b >= 1)
        def _():
            out_copy(b - 1).wait()

        for i in range(3):
            total = keep[v, i, block(q_me), :] + r2[v, 0, i].astype(F32) + r2[v, 1, i].astype(F32)
            outb[i] = total.astype(BF16)
        out_copy(b).start()

    def norm_tile(i):
        rows = pl.ds(pl.multiple_of(i * TE, TE), TE)
        wide = xh[rows, :].astype(F32)
        scale = lax.rsqrt(jnp.mean(wide * wide, -1, keepdims=True) + 1e-6)
        a = (wide * scale).astype(BF16)
        a_ref[rows, :] = a
        across = a.T
        for j in range(N):
            place = ((j % 2 + core) % 2) * (N // 2) + j // 2
            at_ref[pl.ds(place * RD, RD), rows] = across[j * RD : (j + 1) * RD, :]
        acc[rows, :] = jnp.zeros((TE, D), F32)

    def norm_back(i, store):
        rows = pl.ds(pl.multiple_of(i * TE, TE), TE)
        wide = xh[rows, :].astype(F32)
        scale = lax.rsqrt(jnp.mean(wide * wide, -1, keepdims=True) + 1e-6)
        da = acc[rows, :].astype(BF16).astype(F32)
        inner = jnp.mean(da * wide, -1, keepdims=True)
        back = (scale * da - wide * (scale * scale * scale * inner)).astype(BF16)
        store(rows, (dh[rows, :].astype(F32) + back.astype(F32)).astype(BF16))

    def loop(n, f):
        lax.fori_loop(0, n, lambda i, _: (f(i), 0)[1], 0)

    barrier = pltpu.get_barrier_semaphore()
    for dev in (xn, yn, cn):
        pl.semaphore_signal(barrier, inc=1, device_id={"dp": dev}, device_id_type=pl.DeviceIdType.MESH)
    x_copy = pltpu.make_async_copy(x_hbm, xh, io_sem.at[0])
    dy_copy = pltpu.make_async_copy(dy_hbm, dh, io_sem.at[1])
    x_copy.start()
    dy_copy.start()
    pl.semaphore_wait(barrier, 3)
    ag_start(0, (0, 1, 2))
    ag_start(1, (0, 1, 2))
    x_copy.wait()
    loop(T // TE, norm_tile)

    def forward(slot):
        def tile(i):
            rows = pl.ds(pl.multiple_of(i * TT, TT), TT)
            a = a_ref[rows, :]
            gate = dot(a, wgu[slot, 0])
            up = dot(a, wgu[slot, 1])
            p = (gate * jax.nn.sigmoid(gate) * up).astype(BF16)
            acc[rows, :] = acc[rows, :] + dot(p, wdn[slot])

        loop(NT, tile)

    def first(t):
        tick(t)

        @pl.when(t >= 2)
        def _():
            load_wait(t - 2)
            forward(t % 2)

    loop(NC + 2, first)

    def next_state(i):
        rows = pl.ds(pl.multiple_of(i * TE, TE), TE)
        xh[rows, :] = (xh[rows, :].astype(F32) + acc[rows, :].astype(BF16).astype(F32)).astype(BF16)
        norm_tile(i)

    loop(T // TE, next_state)
    dy_copy.wait()

    def backward(s):
        tick(s + NC + 2)
        load_wait(s + NC)
        slot = (s + NC) % 2
        v = s % 2

        @pl.when(s >= 2)
        def _():
            f3(s - 2)

        def tile(i):
            @pl.when((i == 1) & (s >= 1))
            def _():
                f1(s - 1)

            rows = pl.ds(pl.multiple_of(i * TT, TT), TT)
            a = a_ref[rows, :]
            gate = dot(a, wgu[slot, 0])
            up = dot(a, wgu[slot, 1])
            dp = dot_nt(dh[rows, :], wdn[slot]).astype(BF16).astype(F32)
            sig = jax.nn.sigmoid(gate)
            act = gate * sig
            du[rows, :] = (dp * act).astype(BF16)
            dg[rows, :] = (dp * up * (sig + act * (1.0 - sig))).astype(BF16)
            across = (act * up).astype(BF16).T
            for j in range(N):
                place = ((j % 2 + core) % 2) * (N // 2) + j // 2
                pt[pl.ds(place * SEG, SEG), rows] = across[j * SEG : (j + 1) * SEG, :]

        loop(NT, tile)

        @pl.when(s >= 1)
        def _():
            f2(s - 1)
            rs(v, 0).wait_send()

        top, low = pl.ds(0, D // 2), pl.ds(D // 2, D // 2)
        for i, d in enumerate((dg, du)):
            send0[i] = dot(at_ref[low, :], d[...]).astype(BF16)
            keep[v, i] = dot(at_ref[top, :], d[...])
        theirs = dot(pt[pl.ds(HC // 2, HC // 2), :], dh[...]).astype(BF16)
        ours = dot(pt[pl.ds(0, HC // 2), :], dh[...])
        for q in range(N // 2):
            for h in range(2):
                to = pl.ds(q * RD + h * SEG, SEG)
                send0[2, to, :] = theirs[q * SEG : (q + 1) * SEG, h * HC : (h + 1) * HC]
                keep[v, 2, to, :] = ours[q * SEG : (q + 1) * SEG, h * HC : (h + 1) * HC]
        rs(v, 0).start()

        def da_tile(i):
            rows = pl.ds(pl.multiple_of(i * TT, TT), TT)
            acc[rows, :] = acc[rows, :] + (dot_nt(dg[rows, :], wgu[slot, 0]) + dot_nt(du[rows, :], wgu[slot, 1]))

        loop(NT, da_tile)

        @pl.when(s == NC - 1)
        def _():
            def keep_dh(rows, value):
                dh[rows, :] = value

            loop(T // TE, lambda i: norm_back(i, keep_dh))
            again = pltpu.make_async_copy(x_hbm, xh, io_sem.at[0])
            again.start()
            again.wait()
            loop(T // TE, norm_tile)

    loop(K, backward)

    f3(K - 2)
    f1(K - 1)

    def keep_dx(rows, value):
        a_ref[rows, :] = value

    loop(T // TE, lambda i: norm_back(i, keep_dx))
    dx_copy = pltpu.make_async_copy(a_ref, dx_hbm, io_sem.at[1])
    dx_copy.start()
    f2(K - 1)
    f3(K - 1)
    out_copy(K - 1).wait()
    dx_copy.wait()
    for m in range(5):
        rs(1, m).wait_send()

    def drain(k):
        for m in range(8):
            ag(k, m).wait_send()

    loop(K, drain)


def mlp_stack(x, dy, own):
    any_space = pl.BlockSpec(memory_space=pl.ANY)
    vm = pltpu.VMEM
    flops = 19 * 2 * T * D * FF
    return pl.pallas_call(
        kernel,
        name="mlp_stack",
        out_shape=[
            jax.ShapeDtypeStruct((T, D), BF16),
            jax.ShapeDtypeStruct((K, 3, RD, HC), BF16),
            jax.ShapeDtypeStruct((K, N, 3, RD, HC), BF16),
        ],
        in_specs=[any_space] * 3,
        out_specs=[any_space] * 3,
        scratch_shapes=[
            vm((T, D), BF16), vm((T, D), BF16), vm((D, T), BF16), vm((T, D), BF16), vm((T, D), F32),
            vm((2, 2, D, HC), BF16), vm((2, HC, D), BF16),
            vm((HC, T), BF16), vm((T, HC), BF16), vm((T, HC), BF16),
            vm((2, 3, D // 2, HC), F32), vm((3, D // 2, HC), BF16), vm((2, 3, D // 2, HC), BF16),
            vm((2, 3, RD // 2, HC), BF16), vm((2, 2, 3, RD // 2, HC), BF16),
            vm((2, 3, RD, HC), BF16), vm((2, 2, 3, RD, HC), BF16), vm((3, RD, HC), BF16),
            pltpu.SemaphoreType.DMA((K, 8)), pltpu.SemaphoreType.DMA((K, 8)),
            pltpu.SemaphoreType.DMA((5,)), pltpu.SemaphoreType.DMA((2, 5)),
            pltpu.SemaphoreType.DMA((2,)), pltpu.SemaphoreType.DMA((2,)),
            pltpu.SemaphoreType.DMA((2,)), pltpu.SemaphoreType.DMA,
        ],
        compiler_params=pltpu.CompilerParams(
            collective_id=0, has_side_effects=True, vmem_limit_bytes=67_000_000
        ),
        cost_estimate=pl.CostEstimate(flops=flops, bytes_accessed=10**8, transcendentals=T * FF),
    )(x, dy, own)


def solution(mesh):
    def body(x, dy, wg, wu, wd):
        def cut(w):
            return w.reshape(L, RD, N, NC, SEG).transpose(0, 3, 1, 2, 4).reshape(K, RD, HC)

        down = wd.reshape(L, NC, SEG, 2, HC).transpose(0, 1, 3, 2, 4).reshape(K, RD, HC)
        own = jnp.stack([cut(wg), cut(wu), down], axis=1)
        dx, out, _ = mlp_stack(x[0], dy[0], own)

        def join(g):
            return g.reshape(L, NC, RD, N, SEG).transpose(0, 2, 3, 1, 4).reshape(L, RD, FF)

        by_d = out[:, 2].reshape(L, NC, 2, SEG, HC).transpose(0, 1, 3, 2, 4).reshape(L, FF // N, D)
        return dx[None], join(out[:, 0]), join(out[:, 1]), by_d

    act = P(("rep", "dp"), None, None)
    w = P(None, "dp", None)
    return jax.shard_map(
        body, mesh=mesh, in_specs=(act, act, w, w, w), out_specs=(act, *[P("rep", "dp", None)] * 3), check_vma=False
    )
```

```python
import jax
import jax.numpy as jnp
from jax import lax
from jax.experimental import pallas as pl
from jax.experimental.pallas import tpu as pltpu
from jax.sharding import PartitionSpec as P

F32, BF16 = jnp.float32, jnp.bfloat16
T, D, FF, L, N = 2048, 1024, 2560, 2, 8
NC = 5
HC = FF // NC
SEG = HC // N
RD = D // N
K = L * NC
TT = 512
TB = 1024
TE = 256
NN = (((1,), (0,)), ((), ()))
NT_DIMS = (((1,), (1,)), ((), ()))


def dot(a, b):
    return lax.dot_general(a, b, NN, preferred_element_type=F32)


def dot_nt(a, b):
    return lax.dot_general(a, b, NT_DIMS, preferred_element_type=F32)


def kernel(
    x_hbm, dy_hbm, own,
    dx_hbm, out, land, saved,
    xh, a_ref, at_ref, dh, acc, wgu, wdn, pt, dgu, gs,
    keep, mine, send0, recv0, s1, r1, s2, r2, outb,
    ag_send, ag_recv, rs_send, rs_recv, gu_sem, wd_sem, io_sem, out_sem, gs_sem,
):
    me = lax.axis_index("dp")
    core = me % 2
    ypos = (me // 2) % 2
    xpos = me // 4
    xn = (1 - xpos) * 4 + ypos * 2 + core
    yn = xpos * 4 + (1 - ypos) * 2 + core
    cn = xpos * 4 + ypos * 2 + (1 - core)
    diag = (1 - xpos) * 4 + (1 - ypos) * 2 + core
    q_me, q_x, q_y, q_d = me // 2, xn // 2, yn // 2, diag // 2

    def remote(src, dst, ssem, rsem, dev):
        return pltpu.make_async_remote_copy(
            src_ref=src, dst_ref=dst, send_sem=ssem, recv_sem=rsem,
            device_id={"dp": dev}, device_id_type=pl.DeviceIdType.MESH,
        )

    def loop(n, f):
        lax.fori_loop(0, n, lambda i, _: (f(i), 0)[1], 0)

    LO, HI = pl.ds(0, RD // 2), pl.ds(RD // 2, RD // 2)

    def ag(k, m, arriving=False):
        if m < 3:
            dev, src, dst, got = (xn, yn, cn)[m], own.at[k], land.at[k, me], land.at[k, (xn, yn, cn)[m]]
        elif m == 3:
            dev, src, dst, got = yn, land.at[k, xn, :, LO], land.at[k, xn, :, LO], land.at[k, diag, :, LO]
        elif m == 4:
            dev, src, dst, got = xn, land.at[k, yn, :, HI], land.at[k, yn, :, HI], land.at[k, diag, :, HI]
        else:
            b = (xn, yn, diag)[m - 5]
            there = (b // 2) * 2 + (1 - core)
            dev, src, dst, got = cn, land.at[k, b], land.at[k, b], land.at[k, there]
        if arriving:
            src = dst = got
        return remote(src, dst, ag_send.at[k, m], ag_recv.at[k, m], dev)

    def ag_start(k, ms):
        for m in ms:
            ag(k, m).start()

    def ag_wait(k, ms):
        for m in ms:
            ag(k, m, True).wait_recv()

    def load(p):
        k, slot = p % K, p % 2
        for r in range(N):
            if r == 0:
                j, src = me, own.at[k]
            else:
                fx, fy, fc = r // 4, (r // 2) % 2, r % 2
                j = ((xpos + fx) % 2) * 4 + ((ypos + fy) % 2) * 2 + (core + fc) % 2
                src = land.at[k, j]
            rows, segs = pl.ds(j * RD, RD), pl.ds(j * SEG, SEG)
            for h in range(2):
                cols = pl.ds(h * HC, HC)
                pltpu.make_async_copy(src.at[h], wgu.at[slot, rows, cols], gu_sem.at[slot]).start()
                pltpu.make_async_copy(
                    src.at[2, pl.ds(h * SEG, SEG)], wdn.at[slot, segs, cols], wd_sem.at[slot]
                ).start()

    def load_wait(p):
        slot = p % 2
        pltpu.make_async_copy(wgu.at[slot], wgu.at[slot], gu_sem.at[slot]).wait()
        pltpu.make_async_copy(wdn.at[slot], wdn.at[slot], wd_sem.at[slot]).wait()

    def tick(t):
        @pl.when(t < K)
        def _():
            ag_wait(t, (0, 1))
            ag_start(t, (3, 4, 5, 6))

        @pl.when(t + 2 < K)
        def _():
            ag_start(t + 2, (0, 1, 2))

        @pl.when((t >= 1) & (t - 1 < K))
        def _():
            ag_wait(t - 1, (3, 4))
            ag_start(t - 1, (7,))
            ag_wait(t - 1, (2, 5, 6, 7))

        @pl.when((t >= 1) & (t - 1 < K + NC))
        def _():
            load(t - 1)

    def rs(v, m):
        if m < 3:
            src, dst, dev = send0.at[m], recv0.at[v, m], cn
        else:
            i = (m - 3) % 2
            src, dst = (s1.at[i], r1.at[v, i]) if m < 5 else (s2.at[i], r2.at[v, i])
            dev = (xn, yn)[i]
        return remote(src, dst, rs_send.at[m], rs_recv.at[v, m], dev)

    def half(q, h):
        return pl.ds(q * RD + h * (RD // 2), RD // 2)

    def block(q):
        return pl.ds(q * RD, RD)

    def f1(b):
        v = b % 2

        @pl.when(b >= 1)
        def _():
            rs(v, 3).wait_send()
            rs(v, 4).wait_send()

        for i in range(3):
            rs(v, i).wait_recv()
            keep[i] = keep[i] + recv0[v, i].astype(F32)
            s1[0, i] = keep[i, half(q_d, 0), :].astype(BF16)
            s1[1, i] = keep[i, half(q_d, 1), :].astype(BF16)
        rs(v, 3).start()
        rs(v, 4).start()

    def f2(b):
        v = b % 2
        rs(v, 3).wait_recv()
        rs(v, 4).wait_recv()

        @pl.when(b >= 1)
        def _():
            rs(v, 5).wait_send()
            rs(v, 6).wait_send()

        for i in range(3):
            s2[0, i, LO, :] = keep[i, half(q_x, 0), :].astype(BF16)
            s2[0, i, HI, :] = (keep[i, half(q_x, 1), :] + r1[v, 1, i].astype(F32)).astype(BF16)
            s2[1, i, LO, :] = (keep[i, half(q_y, 0), :] + r1[v, 0, i].astype(F32)).astype(BF16)
            s2[1, i, HI, :] = keep[i, half(q_y, 1), :].astype(BF16)
        rs(v, 5).start()
        rs(v, 6).start()
        for i in range(3):
            mine[i] = keep[i, block(q_me), :]

    def out_copy(b):
        return pltpu.make_async_copy(outb, out.at[(b + NC) % K], out_sem)

    def f3(b):
        v = b % 2

        @pl.when(b >= 1)
        def _():
            out_copy(b - 1).wait()

        rs(v, 5).wait_recv()
        rs(v, 6).wait_recv()
        for i in range(3):
            outb[i] = (mine[i] + r2[v, 0, i].astype(F32) + r2[v, 1, i].astype(F32)).astype(BF16)
        out_copy(b).start()

    def some(i, n):
        return pl.ds(pl.multiple_of(i * n, n), n)

    def norm_tile(i):
        rows = some(i, TE)
        wide = xh[rows, :].astype(F32)
        scale = lax.rsqrt(jnp.mean(wide * wide, -1, keepdims=True) + 1e-6)
        a = (wide * scale).astype(BF16)
        a_ref[rows, :] = a
        across = a.T
        for j in range(N):
            place = ((j % 2 + core) % 2) * (N // 2) + j // 2
            at_ref[pl.ds(place * RD, RD), rows] = across[j * RD : (j + 1) * RD, :]
        acc[rows, :] = jnp.zeros((TE, D), F32)

    def norm_back(i, to):
        rows = some(i, TE)
        wide = xh[rows, :].astype(F32)
        scale = lax.rsqrt(jnp.mean(wide * wide, -1, keepdims=True) + 1e-6)
        da = acc[rows, :].astype(BF16).astype(F32)
        inner = jnp.mean(da * wide, -1, keepdims=True)
        back = (scale * da - wide * (scale * scale * scale * inner)).astype(BF16)
        to[rows, :] = (dh[rows, :].astype(F32) + back.astype(F32)).astype(BF16)

    barrier = pltpu.get_barrier_semaphore()
    for dev in (xn, yn, cn):
        pl.semaphore_signal(barrier, inc=1, device_id={"dp": dev}, device_id_type=pl.DeviceIdType.MESH)
    x_copy = pltpu.make_async_copy(x_hbm, xh, io_sem.at[0])
    dy_copy = pltpu.make_async_copy(dy_hbm, dh, io_sem.at[1])
    x_copy.start()
    dy_copy.start()
    pl.semaphore_wait(barrier, 3)
    ag_start(0, (0, 1, 2))
    ag_start(1, (0, 1, 2))
    x_copy.wait()
    loop(T // TE, norm_tile)

    NT = T // TT

    def saving(g):
        return pltpu.make_async_copy(gs.at[g % 2], saved.at[g], gs_sem.at[g % 2])

    def reading(g):
        return pltpu.make_async_copy(saved.at[g], gs.at[g % 2], gs_sem.at[g % 2])

    def first(t):
        tick(t)

        @pl.when(t >= 2)
        def _():
            c, slot = t - 2, t % 2
            load_wait(c)

            def tile(i):
                g = c * NT + i
                rows = some(i, TT)
                both = dot(a_ref[rows, :], wgu[slot])

                @pl.when(g >= 2)
                def _():
                    saving(g - 2).wait()

                gs[g % 2] = both
                saving(g).start()
                gate, up = both[:, :HC], both[:, HC:]
                p = (gate * jax.nn.sigmoid(gate) * up).astype(BF16)
                acc[rows, :] = acc[rows, :] + dot(p, wdn[slot])

            loop(NT, tile)

    loop(NC + 2, first)

    def next_state(i):
        rows = some(i, TE)
        xh[rows, :] = (xh[rows, :].astype(F32) + acc[rows, :].astype(BF16).astype(F32)).astype(BF16)
        norm_tile(i)

    loop(T // TE, next_state)
    dy_copy.wait()
    saving(NC * NT - 2).wait()
    saving(NC * NT - 1).wait()
    reading(0).start()
    reading(1).start()

    def backward(s, n, tile):
        tick(s + NC + 2)
        load_wait(s + NC)
        slot = (s + NC) % 2
        v = s % 2

        def step(i):
            tile(s, i, slot)

            @pl.when((i == 0) & (s >= 1))
            def _():
                f2(s - 1)

        loop(n, step)

        @pl.when(s >= 1)
        def _():
            for m in range(3):
                rs(v, m).wait_send()

        top, low = pl.ds(0, D // 2), pl.ds(D // 2, D // 2)
        both = dot(at_ref[low, :], dgu[...])
        for i in range(2):
            send0[i] = both[:, i * HC : (i + 1) * HC].astype(BF16)
            rs(v, i).start()
        down = dot(pt[pl.ds(HC // 2, HC // 2), :], dh[...])
        for q in range(N // 2):
            for h in range(2):
                to = pl.ds(q * RD + h * SEG, SEG)
                send0[2, to, :] = down[q * SEG : (q + 1) * SEG, h * HC : (h + 1) * HC].astype(BF16)
        rs(v, 2).start()
        both = dot(at_ref[top, :], dgu[...])
        for i in range(2):
            keep[i] = both[:, i * HC : (i + 1) * HC]
        down = dot(pt[pl.ds(0, HC // 2), :], dh[...])
        for q in range(N // 2):
            for h in range(2):
                to = pl.ds(q * RD + h * SEG, SEG)
                keep[2, to, :] = down[q * SEG : (q + 1) * SEG, h * HC : (h + 1) * HC]

        @pl.when(s >= 1)
        def _():
            f3(s - 1)

        f1(s)

        def da_tile(i):
            rows = some(i, TT)
            acc[rows, :] = acc[rows, :] + dot_nt(dgu[rows, :], wgu[slot])

        loop(NT, da_tile)

    def hidden(rows, gate, up, slot):
        dp = dot_nt(dh[rows, :], wdn[slot]).astype(BF16).astype(F32)
        sig = jax.nn.sigmoid(gate)
        act = gate * sig
        dgu[rows, pl.ds(HC, HC)] = (dp * act).astype(BF16)
        dgu[rows, pl.ds(0, HC)] = (dp * up * (sig + act * (1.0 - sig))).astype(BF16)
        across = (act * up).astype(BF16).T
        for j in range(N):
            place = ((j % 2 + core) % 2) * (N // 2) + j // 2
            pt[pl.ds(place * SEG, SEG), rows] = across[j * SEG : (j + 1) * SEG, :]

    def computed(s, i, slot):
        rows = some(i, TB)
        both = dot(a_ref[rows, :], wgu[slot])
        hidden(rows, both[:, :HC], both[:, HC:], slot)

    def read_back(s, i, slot):
        g = (s - NC) * NT + i
        reading(g).wait()
        hidden(some(i, TT), gs[g % 2, :, pl.ds(0, HC)], gs[g % 2, :, pl.ds(HC, HC)], slot)

        @pl.when(g + 2 < NC * NT)
        def _():
            reading(g + 2).start()

    loop(NC, lambda s: backward(s, T // TB, computed))

    def again(i):
        return pltpu.make_async_copy(x_hbm.at[some(i, TE)], xh.at[some(i, TE)], io_sem.at[0])

    def change(i):
        norm_back(i, dh)
        again(i).start()

    loop(T // TE, change)
    x_copy.wait()
    loop(T // TE, norm_tile)
    loop(NC, lambda s: backward(s + NC, NT, read_back))

    f2(K - 1)
    loop(T // TE, lambda i: norm_back(i, a_ref))
    dx_copy = pltpu.make_async_copy(a_ref, dx_hbm, io_sem.at[1])
    dx_copy.start()
    f3(K - 1)
    out_copy(K - 1).wait()
    dx_copy.wait()
    for m in range(7):
        rs(1, m).wait_send()

    def drain(k):
        for m in range(8):
            ag(k, m).wait_send()

    loop(K, drain)


def mlp_stack(x, dy, own):
    any_space = pl.BlockSpec(memory_space=pl.ANY)
    vm = pltpu.VMEM
    flops = 17 * 2 * T * D * FF
    return pl.pallas_call(
        kernel,
        name="mlp_stack",
        out_shape=[
            jax.ShapeDtypeStruct((T, D), BF16),
            jax.ShapeDtypeStruct((K, 3, RD, HC), BF16),
            jax.ShapeDtypeStruct((K, N, 3, RD, HC), BF16),
            jax.ShapeDtypeStruct((NC * (T // TT), TT, 2 * HC), F32),
        ],
        in_specs=[any_space] * 3,
        out_specs=[any_space] * 4,
        scratch_shapes=[
            vm((T, D), BF16), vm((T, D), BF16), vm((D, T), BF16), vm((T, D), BF16), vm((T, D), F32),
            vm((2, D, 2 * HC), BF16), vm((2, HC, D), BF16),
            vm((HC, T), BF16), vm((T, 2 * HC), BF16), vm((2, TT, 2 * HC), F32),
            vm((3, D // 2, HC), F32), vm((3, RD, HC), F32), vm((3, D // 2, HC), BF16), vm((2, 3, D // 2, HC), BF16),
            vm((2, 3, RD // 2, HC), BF16), vm((2, 2, 3, RD // 2, HC), BF16),
            vm((2, 3, RD, HC), BF16), vm((2, 2, 3, RD, HC), BF16), vm((3, RD, HC), BF16),
            pltpu.SemaphoreType.DMA((K, 8)), pltpu.SemaphoreType.DMA((K, 8)),
            pltpu.SemaphoreType.DMA((7,)), pltpu.SemaphoreType.DMA((2, 7)),
            pltpu.SemaphoreType.DMA((2,)), pltpu.SemaphoreType.DMA((2,)),
            pltpu.SemaphoreType.DMA((2,)), pltpu.SemaphoreType.DMA, pltpu.SemaphoreType.DMA((2,)),
        ],
        compiler_params=pltpu.CompilerParams(
            collective_id=0, has_side_effects=True, vmem_limit_bytes=67_000_000
        ),
        cost_estimate=pl.CostEstimate(flops=flops, bytes_accessed=10**8, transcendentals=T * FF),
    )(x, dy, own)


def cut_kernel(wg, wu, wd, own):
    for c in range(NC):
        for i, w in enumerate((wg, wu)):
            parts = [w[0, :, j * (FF // N) + c * SEG : j * (FF // N) + (c + 1) * SEG] for j in range(N)]
            own[c, i] = jnp.concatenate(parts, axis=1)
        for h in range(2):
            own[c, 2, h * SEG : (h + 1) * SEG, :] = wd[0, c * SEG : (c + 1) * SEG, h * HC : (h + 1) * HC]


def cut(wg, wu, wd):
    return pl.pallas_call(
        cut_kernel,
        name="cut",
        grid=(L,),
        out_shape=jax.ShapeDtypeStruct((K, 3, RD, HC), BF16),
        in_specs=[
            pl.BlockSpec((1, RD, FF), lambda n: (n, 0, 0)),
            pl.BlockSpec((1, RD, FF), lambda n: (n, 0, 0)),
            pl.BlockSpec((1, FF // N, D), lambda n: (n, 0, 0)),
        ],
        out_specs=pl.BlockSpec((NC, 3, RD, HC), lambda n: (n, 0, 0, 0)),
    )(wg, wu, wd)


def join_kernel(dx_in, got, dx, wg, wu, wd):
    dx[...] = dx_in[...]
    for i, w in enumerate((wg, wu)):
        parts = [got[c, i, :, j * SEG : (j + 1) * SEG] for j in range(N) for c in range(NC)]
        w[0] = jnp.concatenate(parts, axis=1)
    for c in range(NC):
        for h in range(2):
            wd[0, c * SEG : (c + 1) * SEG, h * HC : (h + 1) * HC] = got[c, 2, h * SEG : (h + 1) * SEG, :]


def join(dx, got):
    return pl.pallas_call(
        join_kernel,
        name="join",
        grid=(L,),
        out_shape=[
            jax.ShapeDtypeStruct((T, D), BF16),
            jax.ShapeDtypeStruct((L, RD, FF), BF16),
            jax.ShapeDtypeStruct((L, RD, FF), BF16),
            jax.ShapeDtypeStruct((L, FF // N, D), BF16),
        ],
        in_specs=[
            pl.BlockSpec((T // L, D), lambda n: (n, 0)),
            pl.BlockSpec((NC, 3, RD, HC), lambda n: (n, 0, 0, 0)),
        ],
        out_specs=[
            pl.BlockSpec((T // L, D), lambda n: (n, 0)),
            pl.BlockSpec((1, RD, FF), lambda n: (n, 0, 0)),
            pl.BlockSpec((1, RD, FF), lambda n: (n, 0, 0)),
            pl.BlockSpec((1, FF // N, D), lambda n: (n, 0, 0)),
        ],
    )(dx, got)


def solution(mesh):
    def body(x, dy, wg, wu, wd):
        dx, got, _, _ = mlp_stack(x[0], dy[0], cut(wg, wu, wd))
        dx, by_g, by_u, by_d = join(dx, got)
        return dx[None], by_g, by_u, by_d

    act = P(("rep", "dp"), None, None)
    w = P(None, "dp", None)
    return jax.shard_map(
        body, mesh=mesh, in_specs=(act, act, w, w, w), out_specs=(act, *[P("rep", "dp", None)] * 3), check_vma=False
    )
```

```python
import jax
import jax.numpy as jnp
from jax import lax
from jax.experimental import pallas as pl
from jax.experimental.pallas import tpu as pltpu
from jax.sharding import PartitionSpec as P

F32, BF16 = jnp.float32, jnp.bfloat16
T, D, FF, L, N = 2048, 1024, 2560, 2, 8
NC = 5
HC = FF // NC
SEG = HC // N
RD = D // N
K = L * NC
TT = 512
TB = 1024
TE = 256
NN = (((1,), (0,)), ((), ()))
NT_DIMS = (((1,), (1,)), ((), ()))


def dot(a, b):
    return lax.dot_general(a, b, NN, preferred_element_type=F32)


def dot_nt(a, b):
    return lax.dot_general(a, b, NT_DIMS, preferred_element_type=F32)


def kernel(
    x_hbm, dy_hbm, own,
    dx_hbm, out, land, saved,
    xh, a_ref, at_ref, dh, acc, wgu, wdn, pt, dgu, gs,
    keep, mine, send0, recv0, s1, r1, s2, r2, outb,
    ag_send, ag_recv, rs_send, rs_recv, gu_sem, wd_sem, io_sem, out_sem, gs_sem,
):
    me = lax.axis_index("dp")
    core = me % 2
    ypos = (me // 2) % 2
    xpos = me // 4
    xn = (1 - xpos) * 4 + ypos * 2 + core
    yn = xpos * 4 + (1 - ypos) * 2 + core
    cn = xpos * 4 + ypos * 2 + (1 - core)
    diag = (1 - xpos) * 4 + (1 - ypos) * 2 + core
    q_me, q_x, q_y, q_d = me // 2, xn // 2, yn // 2, diag // 2

    def remote(src, dst, ssem, rsem, dev):
        return pltpu.make_async_remote_copy(
            src_ref=src, dst_ref=dst, send_sem=ssem, recv_sem=rsem,
            device_id={"dp": dev}, device_id_type=pl.DeviceIdType.MESH,
        )

    def loop(n, f):
        lax.fori_loop(0, n, lambda i, _: (f(i), 0)[1], 0)

    LO, HI = pl.ds(0, RD // 2), pl.ds(RD // 2, RD // 2)

    def ag(k, m, arriving=False):
        if m < 3:
            dev, src, dst, got = (xn, yn, cn)[m], own.at[k], land.at[k, me], land.at[k, (xn, yn, cn)[m]]
        elif m == 3:
            dev, src, dst, got = yn, land.at[k, xn, :, LO], land.at[k, xn, :, LO], land.at[k, diag, :, LO]
        elif m == 4:
            dev, src, dst, got = xn, land.at[k, yn, :, HI], land.at[k, yn, :, HI], land.at[k, diag, :, HI]
        else:
            b = (xn, yn, diag)[m - 5]
            there = (b // 2) * 2 + (1 - core)
            dev, src, dst, got = cn, land.at[k, b], land.at[k, b], land.at[k, there]
        if arriving:
            src = dst = got
        return remote(src, dst, ag_send.at[k, m], ag_recv.at[k, m], dev)

    def ag_start(k, ms):
        for m in ms:
            ag(k, m).start()

    def ag_wait(k, ms):
        for m in ms:
            ag(k, m, True).wait_recv()

    def load(p):
        k, slot = p % K, p % 2
        for r in range(N):
            if r == 0:
                j, src = me, own.at[k]
            else:
                fx, fy, fc = r // 4, (r // 2) % 2, r % 2
                j = ((xpos + fx) % 2) * 4 + ((ypos + fy) % 2) * 2 + (core + fc) % 2
                src = land.at[k, j]
            rows, segs = pl.ds(j * RD, RD), pl.ds(j * SEG, SEG)
            for h in range(2):
                cols = pl.ds(h * HC, HC)
                pltpu.make_async_copy(src.at[h], wgu.at[slot, rows, cols], gu_sem.at[slot]).start()
                pltpu.make_async_copy(
                    src.at[2, pl.ds(h * SEG, SEG)], wdn.at[slot, segs, cols], wd_sem.at[slot]
                ).start()

    def load_wait(p):
        slot = p % 2
        pltpu.make_async_copy(wgu.at[slot], wgu.at[slot], gu_sem.at[slot]).wait()
        pltpu.make_async_copy(wdn.at[slot], wdn.at[slot], wd_sem.at[slot]).wait()

    def begin(k):
        ag_start(k, (0, 1, 2))

    def forward_on(k):
        ag_wait(k, (0, 1))
        ag_start(k, (3, 4, 5, 6))

    def finish(k):
        ag_wait(k, (3, 4))
        ag_start(k, (7,))
        ag_wait(k, (2, 5, 6, 7))

    def rs(v, m):
        if m < 3:
            src, dst, dev = send0.at[m], recv0.at[v, m], cn
        else:
            i = (m - 3) % 2
            src, dst = (s1.at[i], r1.at[v, i]) if m < 5 else (s2.at[i], r2.at[v, i])
            dev = (xn, yn)[i]
        return remote(src, dst, rs_send.at[m], rs_recv.at[v, m], dev)

    def half(q, h):
        return pl.ds(q * RD + h * (RD // 2), RD // 2)

    def block(q):
        return pl.ds(q * RD, RD)

    def f1(b):
        v = b % 2

        @pl.when(b >= 1)
        def _():
            rs(v, 3).wait_send()
            rs(v, 4).wait_send()

        for i in range(3):
            rs(v, i).wait_recv()
            keep[i] = keep[i] + recv0[v, i].astype(F32)
            s1[0, i] = keep[i, half(q_d, 0), :].astype(BF16)
            s1[1, i] = keep[i, half(q_d, 1), :].astype(BF16)
        rs(v, 3).start()
        rs(v, 4).start()

    def f2(b):
        v = b % 2
        rs(v, 3).wait_recv()
        rs(v, 4).wait_recv()

        @pl.when(b >= 1)
        def _():
            rs(v, 5).wait_send()
            rs(v, 6).wait_send()

        for i in range(3):
            s2[0, i, LO, :] = keep[i, half(q_x, 0), :].astype(BF16)
            s2[0, i, HI, :] = (keep[i, half(q_x, 1), :] + r1[v, 1, i].astype(F32)).astype(BF16)
            s2[1, i, LO, :] = (keep[i, half(q_y, 0), :] + r1[v, 0, i].astype(F32)).astype(BF16)
            s2[1, i, HI, :] = keep[i, half(q_y, 1), :].astype(BF16)
        rs(v, 5).start()
        rs(v, 6).start()
        for i in range(3):
            mine[i] = keep[i, block(q_me), :]

    def out_copy(b):
        return pltpu.make_async_copy(outb, out.at[(b + NC) % K], out_sem)

    def f3(b):
        v = b % 2

        @pl.when(b >= 1)
        def _():
            out_copy(b - 1).wait()

        rs(v, 5).wait_recv()
        rs(v, 6).wait_recv()
        for i in range(3):
            outb[i] = (mine[i] + r2[v, 0, i].astype(F32) + r2[v, 1, i].astype(F32)).astype(BF16)
        out_copy(b).start()

    def some(i, n):
        return pl.ds(i * n, n) if isinstance(i, int) else pl.ds(pl.multiple_of(i * n, n), n)

    def norm_tile(i):
        rows = some(i, TE)
        wide = xh[rows, :].astype(F32)
        scale = lax.rsqrt(jnp.mean(wide * wide, -1, keepdims=True) + 1e-6)
        a = (wide * scale).astype(BF16)
        a_ref[rows, :] = a
        across = a.T
        for j in range(N):
            place = ((j % 2 + core) % 2) * (N // 2) + j // 2
            at_ref[pl.ds(place * RD, RD), rows] = across[j * RD : (j + 1) * RD, :]
        acc[rows, :] = jnp.zeros((TE, D), F32)

    def norm_back(i, to):
        rows = some(i, TE)
        wide = xh[rows, :].astype(F32)
        scale = lax.rsqrt(jnp.mean(wide * wide, -1, keepdims=True) + 1e-6)
        da = acc[rows, :].astype(BF16).astype(F32)
        inner = jnp.mean(da * wide, -1, keepdims=True)
        back = (scale * da - wide * (scale * scale * scale * inner)).astype(BF16)
        to[rows, :] = (dh[rows, :].astype(F32) + back.astype(F32)).astype(BF16)

    barrier = pltpu.get_barrier_semaphore()
    for dev in (xn, yn, cn):
        pl.semaphore_signal(barrier, inc=1, device_id={"dp": dev}, device_id_type=pl.DeviceIdType.MESH)
    x_copy = pltpu.make_async_copy(x_hbm, xh, io_sem.at[0])
    dy_copy = pltpu.make_async_copy(dy_hbm, dh, io_sem.at[1])
    x_copy.start()
    dy_copy.start()
    pl.semaphore_wait(barrier, 3)
    begin(0)
    begin(1)
    x_copy.wait()
    loop(T // TE, norm_tile)
    forward_on(0)
    begin(2)

    NT = T // TT

    def saving(g):
        return pltpu.make_async_copy(gs.at[g % 2], saved.at[g], gs_sem.at[g % 2])

    def reading(g):
        return pltpu.make_async_copy(saved.at[g], gs.at[g % 2], gs_sem.at[g % 2])

    def first(c):
        slot = c % 2

        @pl.when(c + 1 < NC)
        def _():
            forward_on(c + 1)

        @pl.when(c + 3 < NC)
        def _():
            begin(c + 3)

        @pl.when(c == NC - 2)
        def _():
            begin(NC)

        finish(c)
        load(c)
        load_wait(c)

        def tile(i):
            @pl.when((c == NC - 1) & (i == NT - 1))
            def _():
                forward_on(NC)
                begin(NC + 1)

            g = c * NT + i
            rows = some(i, TT)
            both = dot(a_ref[rows, :], wgu[slot])

            @pl.when(g >= 2)
            def _():
                saving(g - 2).wait()

            gs[g % 2] = both
            saving(g).start()
            gate, up = both[:, :HC], both[:, HC:]
            p = (gate * jax.nn.sigmoid(gate) * up).astype(BF16)
            acc[rows, :] = acc[rows, :] + dot(p, wdn[slot])

        loop(NT, tile)

    loop(NC, first)

    def next_state(i):
        rows = some(i, TE)
        xh[rows, :] = (xh[rows, :].astype(F32) + acc[rows, :].astype(BF16).astype(F32)).astype(BF16)
        norm_tile(i)

    loop(T // TE, next_state)
    dy_copy.wait()
    saving(NC * NT - 2).wait()
    saving(NC * NT - 1).wait()
    reading(0).start()
    reading(1).start()
    finish(NC)
    load(NC)
    begin(NC + 2)

    def backward(s, n, tile):
        load_wait(s + NC)
        slot = (s + NC) % 2
        v = s % 2

        @pl.when(s + NC + 1 < K)
        def _():
            forward_on(s + NC + 1)

        loop(n, lambda i: tile(s, i, slot))

        @pl.when(s >= 2)
        def _():
            f3(s - 2)

        @pl.when(s >= 1)
        def _():
            f2(s - 1)
            for m in range(3):
                rs(v, m).wait_send()

        @pl.when(s + NC + 3 < K)
        def _():
            begin(s + NC + 3)

        top, low = pl.ds(0, D // 2), pl.ds(D // 2, D // 2)
        both = dot(at_ref[low, :], dgu[...])
        for i in range(2):
            send0[i] = both[:, i * HC : (i + 1) * HC].astype(BF16)
            rs(v, i).start()
        down = dot(pt[pl.ds(HC // 2, HC // 2), :], dh[...])
        for q in range(N // 2):
            for h in range(2):
                to = pl.ds(q * RD + h * SEG, SEG)
                send0[2, to, :] = down[q * SEG : (q + 1) * SEG, h * HC : (h + 1) * HC].astype(BF16)
        rs(v, 2).start()
        both = dot(at_ref[top, :], dgu[...])
        for i in range(2):
            keep[i] = both[:, i * HC : (i + 1) * HC]
        down = dot(pt[pl.ds(0, HC // 2), :], dh[...])
        for q in range(N // 2):
            for h in range(2):
                to = pl.ds(q * RD + h * SEG, SEG)
                keep[2, to, :] = down[q * SEG : (q + 1) * SEG, h * HC : (h + 1) * HC]

        f1(s)

        @pl.when(s + NC + 1 < K)
        def _():
            finish(s + NC + 1)

        @pl.when(s + 1 < K)
        def _():
            load(s + NC + 1)

        def da_tile(i):
            rows = some(i, TT)
            acc[rows, :] = acc[rows, :] + dot_nt(dgu[rows, :], wgu[slot])

        for i in range(NT):
            da_tile(i)

    def hidden(rows, gate, up, slot):
        dp = dot_nt(dh[rows, :], wdn[slot]).astype(BF16).astype(F32)
        sig = jax.nn.sigmoid(gate)
        act = gate * sig
        dgu[rows, pl.ds(HC, HC)] = (dp * act).astype(BF16)
        dgu[rows, pl.ds(0, HC)] = (dp * up * (sig + act * (1.0 - sig))).astype(BF16)
        across = (act * up).astype(BF16).T
        for j in range(N):
            place = ((j % 2 + core) % 2) * (N // 2) + j // 2
            pt[pl.ds(place * SEG, SEG), rows] = across[j * SEG : (j + 1) * SEG, :]

    def computed(s, i, slot):
        rows = some(i, TB)
        both = dot(a_ref[rows, :], wgu[slot])
        hidden(rows, both[:, :HC], both[:, HC:], slot)

    def read_back(s, i, slot):
        g = (s - NC) * NT + i
        reading(g).wait()
        hidden(some(i, TT), gs[g % 2, :, pl.ds(0, HC)], gs[g % 2, :, pl.ds(HC, HC)], slot)

        @pl.when(g + 2 < NC * NT)
        def _():
            reading(g + 2).start()

    loop(NC, lambda s: backward(s, T // TB, computed))

    def again(i):
        return pltpu.make_async_copy(x_hbm.at[some(i, TE)], xh.at[some(i, TE)], io_sem.at[0])

    def change(i):
        norm_back(i, dh)
        again(i).start()

    loop(T // TE, change)
    x_copy.wait()
    loop(T // TE, norm_tile)
    loop(NC, lambda s: backward(s + NC, NT, read_back))

    f3(K - 2)
    f2(K - 1)
    loop(T // TE, lambda i: norm_back(i, a_ref))
    dx_copy = pltpu.make_async_copy(a_ref, dx_hbm, io_sem.at[1])
    dx_copy.start()
    f3(K - 1)
    out_copy(K - 1).wait()
    dx_copy.wait()
    for m in range(7):
        rs(1, m).wait_send()

    def drain(k):
        for m in range(8):
            ag(k, m).wait_send()

    loop(K, drain)


def mlp_stack(x, dy, own):
    any_space = pl.BlockSpec(memory_space=pl.ANY)
    vm = pltpu.VMEM
    flops = 17 * 2 * T * D * FF
    return pl.pallas_call(
        kernel,
        name="mlp_stack",
        out_shape=[
            jax.ShapeDtypeStruct((T, D), BF16),
            jax.ShapeDtypeStruct((K, 3, RD, HC), BF16),
            jax.ShapeDtypeStruct((K, N, 3, RD, HC), BF16),
            jax.ShapeDtypeStruct((NC * (T // TT), TT, 2 * HC), F32),
        ],
        in_specs=[any_space] * 3,
        out_specs=[any_space] * 4,
        scratch_shapes=[
            vm((T, D), BF16), vm((T, D), BF16), vm((D, T), BF16), vm((T, D), BF16), vm((T, D), F32),
            vm((2, D, 2 * HC), BF16), vm((2, HC, D), BF16),
            vm((HC, T), BF16), vm((T, 2 * HC), BF16), vm((2, TT, 2 * HC), F32),
            vm((3, D // 2, HC), F32), vm((3, RD, HC), F32), vm((3, D // 2, HC), BF16), vm((2, 3, D // 2, HC), BF16),
            vm((2, 3, RD // 2, HC), BF16), vm((2, 2, 3, RD // 2, HC), BF16),
            vm((2, 3, RD, HC), BF16), vm((2, 2, 3, RD, HC), BF16), vm((3, RD, HC), BF16),
            pltpu.SemaphoreType.DMA((K, 8)), pltpu.SemaphoreType.DMA((K, 8)),
            pltpu.SemaphoreType.DMA((7,)), pltpu.SemaphoreType.DMA((2, 7)),
            pltpu.SemaphoreType.DMA((2,)), pltpu.SemaphoreType.DMA((2,)),
            pltpu.SemaphoreType.DMA((2,)), pltpu.SemaphoreType.DMA, pltpu.SemaphoreType.DMA((2,)),
        ],
        compiler_params=pltpu.CompilerParams(
            collective_id=0, has_side_effects=True, vmem_limit_bytes=67_000_000
        ),
        cost_estimate=pl.CostEstimate(flops=flops, bytes_accessed=10**8, transcendentals=T * FF),
    )(x, dy, own)


def cut_kernel(wg, wu, wd, own):
    for c in range(NC):
        for i, w in enumerate((wg, wu)):
            parts = [w[0, :, j * (FF // N) + c * SEG : j * (FF // N) + (c + 1) * SEG] for j in range(N)]
            own[c, i] = jnp.concatenate(parts, axis=1)
        for h in range(2):
            own[c, 2, h * SEG : (h + 1) * SEG, :] = wd[0, c * SEG : (c + 1) * SEG, h * HC : (h + 1) * HC]


def cut(wg, wu, wd):
    return pl.pallas_call(
        cut_kernel,
        name="cut",
        grid=(L,),
        out_shape=jax.ShapeDtypeStruct((K, 3, RD, HC), BF16),
        in_specs=[
            pl.BlockSpec((1, RD, FF), lambda n: (n, 0, 0)),
            pl.BlockSpec((1, RD, FF), lambda n: (n, 0, 0)),
            pl.BlockSpec((1, FF // N, D), lambda n: (n, 0, 0)),
        ],
        out_specs=pl.BlockSpec((NC, 3, RD, HC), lambda n: (n, 0, 0, 0)),
    )(wg, wu, wd)


def join_kernel(dx_in, got, dx, wg, wu, wd):
    dx[...] = dx_in[...]
    for i, w in enumerate((wg, wu)):
        parts = [got[c, i, :, j * SEG : (j + 1) * SEG] for j in range(N) for c in range(NC)]
        w[0] = jnp.concatenate(parts, axis=1)
    for c in range(NC):
        for h in range(2):
            wd[0, c * SEG : (c + 1) * SEG, h * HC : (h + 1) * HC] = got[c, 2, h * SEG : (h + 1) * SEG, :]


def join(dx, got):
    return pl.pallas_call(
        join_kernel,
        name="join",
        grid=(L,),
        out_shape=[
            jax.ShapeDtypeStruct((T, D), BF16),
            jax.ShapeDtypeStruct((L, RD, FF), BF16),
            jax.ShapeDtypeStruct((L, RD, FF), BF16),
            jax.ShapeDtypeStruct((L, FF // N, D), BF16),
        ],
        in_specs=[
            pl.BlockSpec((T // L, D), lambda n: (n, 0)),
            pl.BlockSpec((NC, 3, RD, HC), lambda n: (n, 0, 0, 0)),
        ],
        out_specs=[
            pl.BlockSpec((T // L, D), lambda n: (n, 0)),
            pl.BlockSpec((1, RD, FF), lambda n: (n, 0, 0)),
            pl.BlockSpec((1, RD, FF), lambda n: (n, 0, 0)),
            pl.BlockSpec((1, FF // N, D), lambda n: (n, 0, 0)),
        ],
    )(dx, got)


def solution(mesh):
    def body(x, dy, wg, wu, wd):
        dx, got, _, _ = mlp_stack(x[0], dy[0], cut(wg, wu, wd))
        dx, by_g, by_u, by_d = join(dx, got)
        return dx[None], by_g, by_u, by_d

    act = P(("rep", "dp"), None, None)
    w = P(None, "dp", None)
    return jax.shard_map(
        body, mesh=mesh, in_specs=(act, act, w, w, w), out_specs=(act, *[P("rep", "dp", None)] * 3), check_vma=False
    )
```

```python
import jax
import jax.numpy as jnp
from jax import lax
from jax.experimental import pallas as pl
from jax.experimental.pallas import tpu as pltpu
from jax.sharding import PartitionSpec as P

F32, BF16 = jnp.float32, jnp.bfloat16
T, D, FF, L, N = 2048, 1024, 2560, 2, 8
NC = 5
HC = FF // NC
SEG = HC // N
RD = D // N
K = L * NC
TT = 512
TB = 1024
TE = 256
NN = (((1,), (0,)), ((), ()))
NT_DIMS = (((1,), (1,)), ((), ()))


def dot(a, b):
    return lax.dot_general(a, b, NN, preferred_element_type=F32)


def dot_nt(a, b):
    return lax.dot_general(a, b, NT_DIMS, preferred_element_type=F32)


def kernel(
    x_hbm, dy_hbm, own,
    dx_hbm, out, land, saved, saved_p, saved_a, saved_at,
    xh, a_ref, at_ref, dh, acc, wgu, wdn, pt, dgu, gs,
    keep, mine, send0, recv0, s1, r1, s2, r2, outb,
    ag_send, ag_recv, rs_send, rs_recv, gu_sem, wd_sem, io_sem, out_sem, gs_sem, pt_sem,
):
    me = lax.axis_index("dp")
    core = me % 2
    ypos = (me // 2) % 2
    xpos = me // 4
    xn = (1 - xpos) * 4 + ypos * 2 + core
    yn = xpos * 4 + (1 - ypos) * 2 + core
    cn = xpos * 4 + ypos * 2 + (1 - core)
    diag = (1 - xpos) * 4 + (1 - ypos) * 2 + core
    q_me, q_x, q_y, q_d = me // 2, xn // 2, yn // 2, diag // 2

    def remote(src, dst, ssem, rsem, dev):
        return pltpu.make_async_remote_copy(
            src_ref=src, dst_ref=dst, send_sem=ssem, recv_sem=rsem,
            device_id={"dp": dev}, device_id_type=pl.DeviceIdType.MESH,
        )

    def loop(n, f):
        lax.fori_loop(0, n, lambda i, _: (f(i), 0)[1], 0)

    LO, HI = pl.ds(0, RD // 2), pl.ds(RD // 2, RD // 2)

    def ag(k, m, arriving=False):
        if m < 3:
            dev, src, dst, got = (xn, yn, cn)[m], own.at[k], land.at[k, me], land.at[k, (xn, yn, cn)[m]]
        elif m == 3:
            dev, src, dst, got = yn, land.at[k, xn, :, LO], land.at[k, xn, :, LO], land.at[k, diag, :, LO]
        elif m == 4:
            dev, src, dst, got = xn, land.at[k, yn, :, HI], land.at[k, yn, :, HI], land.at[k, diag, :, HI]
        else:
            b = (xn, yn, diag)[m - 5]
            there = (b // 2) * 2 + (1 - core)
            dev, src, dst, got = cn, land.at[k, b], land.at[k, b], land.at[k, there]
        if arriving:
            src = dst = got
        return remote(src, dst, ag_send.at[k, m], ag_recv.at[k, m], dev)

    def ag_start(k, ms):
        for m in ms:
            ag(k, m).start()

    def ag_wait(k, ms):
        for m in ms:
            ag(k, m, True).wait_recv()

    def load(p):
        k, slot = p % K, p % 2
        for r in range(N):
            if r == 0:
                j, src = me, own.at[k]
            else:
                fx, fy, fc = r // 4, (r // 2) % 2, r % 2
                j = ((xpos + fx) % 2) * 4 + ((ypos + fy) % 2) * 2 + (core + fc) % 2
                src = land.at[k, j]
            rows, segs = pl.ds(j * RD, RD), pl.ds(j * SEG, SEG)
            for h in range(2):
                cols = pl.ds(h * HC, HC)
                pltpu.make_async_copy(src.at[h], wgu.at[slot, rows, cols], gu_sem.at[slot]).start()
                pltpu.make_async_copy(
                    src.at[2, pl.ds(h * SEG, SEG)], wdn.at[slot, segs, cols], wd_sem.at[slot]
                ).start()

    def load_wait(p):
        slot = p % 2
        pltpu.make_async_copy(wgu.at[slot], wgu.at[slot], gu_sem.at[slot]).wait()
        pltpu.make_async_copy(wdn.at[slot], wdn.at[slot], wd_sem.at[slot]).wait()

    def begin(k):
        ag_start(k, (0, 1, 2))

    def forward_on(k):
        ag_wait(k, (0, 1))
        ag_start(k, (3, 4, 5, 6))

    def finish(k):
        ag_wait(k, (3, 4))
        ag_start(k, (7,))
        ag_wait(k, (2, 5, 6, 7))

    def rs(v, m):
        if m < 3:
            src, dst, dev = send0.at[m], recv0.at[v, m], cn
        else:
            i = (m - 3) % 2
            src, dst = (s1.at[i], r1.at[v, i]) if m < 5 else (s2.at[i], r2.at[v, i])
            dev = (xn, yn)[i]
        return remote(src, dst, rs_send.at[m], rs_recv.at[v, m], dev)

    def half(q, h):
        return pl.ds(q * RD + h * (RD // 2), RD // 2)

    def block(q):
        return pl.ds(q * RD, RD)

    def f1(b):
        v = b % 2

        @pl.when(b >= 1)
        def _():
            rs(v, 3).wait_send()
            rs(v, 4).wait_send()

        for i in range(3):
            rs(v, i).wait_recv()
            keep[i] = keep[i] + recv0[v, i].astype(F32)
            s1[0, i] = keep[i, half(q_d, 0), :].astype(BF16)
            s1[1, i] = keep[i, half(q_d, 1), :].astype(BF16)
        rs(v, 3).start()
        rs(v, 4).start()

    def f2(b):
        v = b % 2
        rs(v, 3).wait_recv()
        rs(v, 4).wait_recv()

        @pl.when(b >= 1)
        def _():
            rs(v, 5).wait_send()
            rs(v, 6).wait_send()

        for i in range(3):
            s2[0, i, LO, :] = keep[i, half(q_x, 0), :].astype(BF16)
            s2[0, i, HI, :] = (keep[i, half(q_x, 1), :] + r1[v, 1, i].astype(F32)).astype(BF16)
            s2[1, i, LO, :] = (keep[i, half(q_y, 0), :] + r1[v, 0, i].astype(F32)).astype(BF16)
            s2[1, i, HI, :] = keep[i, half(q_y, 1), :].astype(BF16)
        rs(v, 5).start()
        rs(v, 6).start()
        for i in range(3):
            mine[i] = keep[i, block(q_me), :]

    def out_copy(b):
        return pltpu.make_async_copy(outb, out.at[(b + NC) % K], out_sem)

    def f3(b):
        v = b % 2

        @pl.when(b >= 1)
        def _():
            out_copy(b - 1).wait()

        rs(v, 5).wait_recv()
        rs(v, 6).wait_recv()
        for i in range(3):
            outb[i] = (mine[i] + r2[v, 0, i].astype(F32) + r2[v, 1, i].astype(F32)).astype(BF16)
        out_copy(b).start()

    def some(i, n):
        return pl.ds(i * n, n) if isinstance(i, int) else pl.ds(pl.multiple_of(i * n, n), n)

    def norm_tile(i):
        rows = some(i, TE)
        wide = xh[rows, :].astype(F32)
        scale = lax.rsqrt(jnp.mean(wide * wide, -1, keepdims=True) + 1e-6)
        a = (wide * scale).astype(BF16)
        a_ref[rows, :] = a
        across = a.T
        for j in range(N):
            place = ((j % 2 + core) % 2) * (N // 2) + j // 2
            at_ref[pl.ds(place * RD, RD), rows] = across[j * RD : (j + 1) * RD, :]
        acc[rows, :] = jnp.zeros((TE, D), F32)

    def norm_back(i, to):
        rows = some(i, TE)
        wide = xh[rows, :].astype(F32)
        scale = lax.rsqrt(jnp.mean(wide * wide, -1, keepdims=True) + 1e-6)
        da = acc[rows, :].astype(BF16).astype(F32)
        inner = jnp.mean(da * wide, -1, keepdims=True)
        back = (scale * da - wide * (scale * scale * scale * inner)).astype(BF16)
        to[rows, :] = (dh[rows, :].astype(F32) + back.astype(F32)).astype(BF16)

    barrier = pltpu.get_barrier_semaphore()
    for dev in (xn, yn, cn):
        pl.semaphore_signal(barrier, inc=1, device_id={"dp": dev}, device_id_type=pl.DeviceIdType.MESH)
    x_copy = pltpu.make_async_copy(x_hbm, xh, io_sem.at[0])
    dy_copy = pltpu.make_async_copy(dy_hbm, dh, io_sem.at[1])
    x_copy.start()
    dy_copy.start()
    pl.semaphore_wait(barrier, 3)
    begin(0)
    begin(1)
    x_copy.wait()
    loop(T // TE, norm_tile)
    a_out = pltpu.make_async_copy(a_ref, saved_a, io_sem.at[2])
    at_out = pltpu.make_async_copy(at_ref, saved_at, io_sem.at[3])
    a_out.start()
    at_out.start()
    forward_on(0)
    begin(2)

    NT = T // TT

    def silu(both):
        gate, up = both[:, :HC], both[:, HC:]
        sig = jax.nn.sigmoid(gate)
        act = gate * sig
        return act, sig + act * (1.0 - sig), up

    def put_p(p, rows):
        across = p.T
        for j in range(N):
            place = ((j % 2 + core) % 2) * (N // 2) + j // 2
            pt[pl.ds(place * SEG, SEG), rows] = across[j * SEG : (j + 1) * SEG, :]

    def saving(g):
        return pltpu.make_async_copy(gs.at[g % 2], saved.at[g], gs_sem.at[g % 2])

    def reading(g):
        return pltpu.make_async_copy(saved.at[g], gs.at[g % 2], gs_sem.at[g % 2])

    def keep_p(c):
        return pltpu.make_async_copy(pt, saved_p.at[c], pt_sem)

    def first(c):
        slot = c % 2

        @pl.when(c + 1 < NC)
        def _():
            forward_on(c + 1)

        @pl.when(c + 3 < NC)
        def _():
            begin(c + 3)

        @pl.when(c == NC - 2)
        def _():
            begin(NC)

        @pl.when(c < NC - 1)
        def _():
            finish(c)
            load(c)

        load_wait(c)

        def tile(i):
            @pl.when((c == NC - 2) & (i == NT - 2))
            def _():
                finish(NC - 1)
                load(NC - 1)

            @pl.when((c == NC - 1) & (i == NT - 2))
            def _():
                forward_on(NC)
                begin(NC + 1)
                begin(NC + 2)

            g = c * NT + i

            @pl.when(g >= 2)
            def _():
                saving(g - 2).wait()

            @pl.when((c >= 1) & (i == 0))
            def _():
                keep_p(c - 1).wait()

            rows = some(i, TT)
            both = dot(a_ref[rows, :], wgu[slot])
            act, slope, up = silu(both)
            gs[g % 2, :, pl.ds(0, HC)] = act
            gs[g % 2, :, pl.ds(HC, HC)] = slope * up
            saving(g).start()
            p = (act * up).astype(BF16)
            put_p(p, rows)
            acc[rows, :] = acc[rows, :] + dot(p, wdn[slot])

        loop(NT, tile)
        keep_p(c).start()

    loop(NC, first)

    def next_state(i):
        rows = some(i, TE)
        xh[rows, :] = (xh[rows, :].astype(F32) + acc[rows, :].astype(BF16).astype(F32)).astype(BF16)
        norm_tile(i)

    a_out.wait()
    at_out.wait()
    loop(T // TE, next_state)
    dy_copy.wait()
    keep_p(NC - 1).wait()
    saving(NC * NT - 2).wait()
    saving(NC * NT - 1).wait()
    reading(0).start()
    reading(1).start()
    finish(NC)
    load(NC)

    def get_p(c):
        return pltpu.make_async_copy(saved_p.at[c], pt, pt_sem)

    a_in = pltpu.make_async_copy(saved_a, a_ref, io_sem.at[2])
    at_in = pltpu.make_async_copy(saved_at, at_ref, io_sem.at[3])

    def backward(s, n, tile):
        load_wait(s + NC)
        slot = (s + NC) % 2
        v = s % 2

        @pl.when((s >= 1) & (s + NC + 1 < K))
        def _():
            forward_on(s + NC + 1)

        loop(n, lambda i: tile(s, i, slot))

        @pl.when(s >= 2)
        def _():
            f3(s - 2)

        @pl.when(s >= 1)
        def _():
            f2(s - 1)
            for m in range(3):
                rs(v, m).wait_send()

        @pl.when(s == 0)
        def _():
            forward_on(NC + 1)

        @pl.when(s + NC + 3 < K)
        def _():
            begin(s + NC + 3)

        @pl.when(s >= NC)
        def _():
            get_p(s - NC).wait()

        top, low = pl.ds(0, D // 2), pl.ds(D // 2, D // 2)
        both = dot(at_ref[low, :], dgu[...])
        for i in range(2):
            send0[i] = both[:, i * HC : (i + 1) * HC].astype(BF16)
            rs(v, i).start()
        down = dot(pt[pl.ds(HC // 2, HC // 2), :], dh[...])
        for q in range(N // 2):
            for h in range(2):
                to = pl.ds(q * RD + h * SEG, SEG)
                send0[2, to, :] = down[q * SEG : (q + 1) * SEG, h * HC : (h + 1) * HC].astype(BF16)
        rs(v, 2).start()
        both = dot(at_ref[top, :], dgu[...])
        for i in range(2):
            keep[i] = both[:, i * HC : (i + 1) * HC]
        down = dot(pt[pl.ds(0, HC // 2), :], dh[...])
        for q in range(N // 2):
            for h in range(2):
                to = pl.ds(q * RD + h * SEG, SEG)
                keep[2, to, :] = down[q * SEG : (q + 1) * SEG, h * HC : (h + 1) * HC]

        @pl.when((s >= NC - 1) & (s + 1 < K))
        def _():
            get_p(s + 1 - NC).start()

        @pl.when(s == NC - 1)
        def _():
            a_in.start()
            at_in.start()

        f1(s)

        @pl.when(s + NC + 1 < K)
        def _():
            finish(s + NC + 1)

        @pl.when(s + 1 < K)
        def _():
            load(s + NC + 1)

        def da_tile(i):
            rows = some(i, TT)
            acc[rows, :] = acc[rows, :] + dot_nt(dgu[rows, :], wgu[slot])

        for i in range(NT):
            da_tile(i)

    def back_to(rows, act, slope, slot):
        dp = dot_nt(dh[rows, :], wdn[slot]).astype(BF16).astype(F32)
        dgu[rows, pl.ds(HC, HC)] = (dp * act).astype(BF16)
        dgu[rows, pl.ds(0, HC)] = (dp * slope).astype(BF16)

    def computed(s, i, slot):
        rows = some(i, TB)
        act, slope, up = silu(dot(a_ref[rows, :], wgu[slot]))
        back_to(rows, act, slope * up, slot)
        put_p((act * up).astype(BF16), rows)

    def read_back(s, i, slot):
        g = (s - NC) * NT + i
        reading(g).wait()
        back_to(some(i, TT), gs[g % 2, :, pl.ds(0, HC)], gs[g % 2, :, pl.ds(HC, HC)], slot)

        @pl.when(g + 2 < NC * NT)
        def _():
            reading(g + 2).start()

    loop(NC, lambda s: backward(s, T // TB, computed))

    def change(i):
        norm_back(i, dh)
        rows = some(i, TE)
        acc[rows, :] = jnp.zeros((TE, D), F32)

    loop(T // TE, change)
    x_again = pltpu.make_async_copy(x_hbm, xh, io_sem.at[0])
    x_again.start()
    a_in.wait()
    at_in.wait()
    loop(NC, lambda s: backward(s + NC, NT, read_back))

    x_again.wait()
    f3(K - 2)
    f2(K - 1)
    loop(T // TE, lambda i: norm_back(i, a_ref))
    dx_copy = pltpu.make_async_copy(a_ref, dx_hbm, io_sem.at[1])
    dx_copy.start()
    f3(K - 1)
    out_copy(K - 1).wait()
    dx_copy.wait()
    for m in range(7):
        rs(1, m).wait_send()

    def drain(k):
        for m in range(8):
            ag(k, m).wait_send()

    loop(K, drain)


def mlp_stack(x, dy, own):
    any_space = pl.BlockSpec(memory_space=pl.ANY)
    vm = pltpu.VMEM
    flops = 17 * 2 * T * D * FF
    return pl.pallas_call(
        kernel,
        name="mlp_stack",
        out_shape=[
            jax.ShapeDtypeStruct((T, D), BF16),
            jax.ShapeDtypeStruct((K, 3, RD, HC), BF16),
            jax.ShapeDtypeStruct((K, N, 3, RD, HC), BF16),
            jax.ShapeDtypeStruct((NC * (T // TT), TT, 2 * HC), F32),
            jax.ShapeDtypeStruct((NC, HC, T), BF16),
            jax.ShapeDtypeStruct((T, D), BF16),
            jax.ShapeDtypeStruct((D, T), BF16),
        ],
        in_specs=[any_space] * 3,
        out_specs=[any_space] * 7,
        scratch_shapes=[
            vm((T, D), BF16), vm((T, D), BF16), vm((D, T), BF16), vm((T, D), BF16), vm((T, D), F32),
            vm((2, D, 2 * HC), BF16), vm((2, HC, D), BF16),
            vm((HC, T), BF16), vm((T, 2 * HC), BF16), vm((2, TT, 2 * HC), F32),
            vm((3, D // 2, HC), F32), vm((3, RD, HC), F32), vm((3, D // 2, HC), BF16), vm((2, 3, D // 2, HC), BF16),
            vm((2, 3, RD // 2, HC), BF16), vm((2, 2, 3, RD // 2, HC), BF16),
            vm((2, 3, RD, HC), BF16), vm((2, 2, 3, RD, HC), BF16), vm((3, RD, HC), BF16),
            pltpu.SemaphoreType.DMA((K, 8)), pltpu.SemaphoreType.DMA((K, 8)),
            pltpu.SemaphoreType.DMA((7,)), pltpu.SemaphoreType.DMA((2, 7)),
            pltpu.SemaphoreType.DMA((2,)), pltpu.SemaphoreType.DMA((2,)),
            pltpu.SemaphoreType.DMA((4,)), pltpu.SemaphoreType.DMA, pltpu.SemaphoreType.DMA((2,)), pltpu.SemaphoreType.DMA,
        ],
        compiler_params=pltpu.CompilerParams(
            collective_id=0, has_side_effects=True, vmem_limit_bytes=67_000_000
        ),
        cost_estimate=pl.CostEstimate(flops=flops, bytes_accessed=10**8, transcendentals=T * FF),
    )(x, dy, own)


def cut_kernel(wg, wu, wd, own):
    for c in range(NC):
        for i, w in enumerate((wg, wu)):
            parts = [w[0, :, j * (FF // N) + c * SEG : j * (FF // N) + (c + 1) * SEG] for j in range(N)]
            own[c, i] = jnp.concatenate(parts, axis=1)
        for h in range(2):
            own[c, 2, h * SEG : (h + 1) * SEG, :] = wd[0, c * SEG : (c + 1) * SEG, h * HC : (h + 1) * HC]


def cut(wg, wu, wd):
    return pl.pallas_call(
        cut_kernel,
        name="cut",
        grid=(L,),
        out_shape=jax.ShapeDtypeStruct((K, 3, RD, HC), BF16),
        in_specs=[
            pl.BlockSpec((1, RD, FF), lambda n: (n, 0, 0)),
            pl.BlockSpec((1, RD, FF), lambda n: (n, 0, 0)),
            pl.BlockSpec((1, FF // N, D), lambda n: (n, 0, 0)),
        ],
        out_specs=pl.BlockSpec((NC, 3, RD, HC), lambda n: (n, 0, 0, 0)),
    )(wg, wu, wd)


def join_kernel(dx_in, got, dx, wg, wu, wd):
    dx[...] = dx_in[...]
    for i, w in enumerate((wg, wu)):
        parts = [got[c, i, :, j * SEG : (j + 1) * SEG] for j in range(N) for c in range(NC)]
        w[0] = jnp.concatenate(parts, axis=1)
    for c in range(NC):
        for h in range(2):
            wd[0, c * SEG : (c + 1) * SEG, h * HC : (h + 1) * HC] = got[c, 2, h * SEG : (h + 1) * SEG, :]


def join(dx, got):
    return pl.pallas_call(
        join_kernel,
        name="join",
        grid=(L,),
        out_shape=[
            jax.ShapeDtypeStruct((T, D), BF16),
            jax.ShapeDtypeStruct((L, RD, FF), BF16),
            jax.ShapeDtypeStruct((L, RD, FF), BF16),
            jax.ShapeDtypeStruct((L, FF // N, D), BF16),
        ],
        in_specs=[
            pl.BlockSpec((T // L, D), lambda n: (n, 0)),
            pl.BlockSpec((NC, 3, RD, HC), lambda n: (n, 0, 0, 0)),
        ],
        out_specs=[
            pl.BlockSpec((T // L, D), lambda n: (n, 0)),
            pl.BlockSpec((1, RD, FF), lambda n: (n, 0, 0)),
            pl.BlockSpec((1, RD, FF), lambda n: (n, 0, 0)),
            pl.BlockSpec((1, FF // N, D), lambda n: (n, 0, 0)),
        ],
    )(dx, got)


def solution(mesh):
    def body(x, dy, wg, wu, wd):
        dx, got, *_ = mlp_stack(x[0], dy[0], cut(wg, wu, wd))
        dx, by_g, by_u, by_d = join(dx, got)
        return dx[None], by_g, by_u, by_d

    act = P(("rep", "dp"), None, None)
    w = P(None, "dp", None)
    return jax.shard_map(
        body, mesh=mesh, in_specs=(act, act, w, w, w), out_specs=(act, *[P("rep", "dp", None)] * 3), check_vma=False
    )
```

```python
import jax
import jax.numpy as jnp
from jax import lax
from jax.experimental import pallas as pl
from jax.experimental.pallas import tpu as pltpu
from jax.sharding import PartitionSpec as P

F32, BF16 = jnp.float32, jnp.bfloat16
T, D, FF, L, N = 2048, 1024, 2560, 2, 8
NC = 5
HC = FF // NC
SEG = HC // N
RD = D // N
K = L * NC
TT = 512
TB = 1024
TE = 256
NN = (((1,), (0,)), ((), ()))
NT_DIMS = (((1,), (1,)), ((), ()))


def dot(a, b):
    return lax.dot_general(a, b, NN, preferred_element_type=F32)


def dot_nt(a, b):
    return lax.dot_general(a, b, NT_DIMS, preferred_element_type=F32)


def kernel(
    x_hbm, dy_hbm, own,
    dx_hbm, out, land, saved, saved_p, saved_at,
    xh, two, at_ref, dh, acc, wgu, wdn, pt, gs,
    keep, mine, send0, recv0, s1, r1, s2, r2, outb,
    ag_send, ag_recv, rs_send, rs_recv, gu_sem, wd_sem, io_sem, out_sem, gs_sem, pt_sem,
):
    a_ref, dgu = two.at[0], two.at[1]
    me = lax.axis_index("dp")
    core = me % 2
    ypos = (me // 2) % 2
    xpos = me // 4
    xn = (1 - xpos) * 4 + ypos * 2 + core
    yn = xpos * 4 + (1 - ypos) * 2 + core
    cn = xpos * 4 + ypos * 2 + (1 - core)
    diag = (1 - xpos) * 4 + (1 - ypos) * 2 + core
    q_me, q_x, q_y, q_d = me // 2, xn // 2, yn // 2, diag // 2

    def remote(src, dst, ssem, rsem, dev):
        return pltpu.make_async_remote_copy(
            src_ref=src, dst_ref=dst, send_sem=ssem, recv_sem=rsem,
            device_id={"dp": dev}, device_id_type=pl.DeviceIdType.MESH,
        )

    def loop(n, f):
        lax.fori_loop(0, n, lambda i, _: (f(i), 0)[1], 0)

    LO, HI = pl.ds(0, RD // 2), pl.ds(RD // 2, RD // 2)

    def ag(k, m, arriving=False):
        if m < 3:
            dev, src, dst, got = (xn, yn, cn)[m], own.at[k], land.at[k, me], land.at[k, (xn, yn, cn)[m]]
        elif m == 3:
            dev, src, dst, got = yn, land.at[k, xn, :, LO], land.at[k, xn, :, LO], land.at[k, diag, :, LO]
        elif m == 4:
            dev, src, dst, got = xn, land.at[k, yn, :, HI], land.at[k, yn, :, HI], land.at[k, diag, :, HI]
        else:
            b = (xn, yn, diag)[m - 5]
            there = (b // 2) * 2 + (1 - core)
            dev, src, dst, got = cn, land.at[k, b], land.at[k, b], land.at[k, there]
        if arriving:
            src = dst = got
        return remote(src, dst, ag_send.at[k, m], ag_recv.at[k, m], dev)

    def ag_start(k, ms):
        for m in ms:
            ag(k, m).start()

    def ag_wait(k, ms):
        for m in ms:
            ag(k, m, True).wait_recv()

    def load(p):
        k, slot = p % K, p % 2
        for r in range(N):
            if r == 0:
                j, src = me, own.at[k]
            else:
                fx, fy, fc = r // 4, (r // 2) % 2, r % 2
                j = ((xpos + fx) % 2) * 4 + ((ypos + fy) % 2) * 2 + (core + fc) % 2
                src = land.at[k, j]
            rows, segs = pl.ds(j * RD, RD), pl.ds(j * SEG, SEG)
            for h in range(2):
                cols = pl.ds(h * HC, HC)
                pltpu.make_async_copy(src.at[h], wgu.at[slot, rows, cols], gu_sem.at[slot]).start()
                pltpu.make_async_copy(
                    src.at[2, pl.ds(h * SEG, SEG)], wdn.at[slot, segs, cols], wd_sem.at[slot]
                ).start()

    def load_wait(p):
        slot = p % 2
        pltpu.make_async_copy(wgu.at[slot], wgu.at[slot], gu_sem.at[slot]).wait()
        pltpu.make_async_copy(wdn.at[slot], wdn.at[slot], wd_sem.at[slot]).wait()

    def begin(k):
        ag_start(k, (0, 1, 2))

    def forward_on(k):
        ag_wait(k, (0, 1))
        ag_start(k, (3, 4, 5, 6))

    def finish(k):
        ag_wait(k, (3, 4))
        ag_start(k, (7,))
        ag_wait(k, (2, 5, 6, 7))

    def rs(v, m):
        if m < 3:
            src, dst, dev = send0.at[m], recv0.at[v, m], cn
        else:
            i = (m - 3) % 2
            src, dst = (s1.at[i], r1.at[v, i]) if m < 5 else (s2.at[i], r2.at[v, i])
            dev = (xn, yn)[i]
        return remote(src, dst, rs_send.at[m], rs_recv.at[v, m], dev)

    def half(q, h):
        return pl.ds(q * RD + h * (RD // 2), RD // 2)

    def block(q):
        return pl.ds(q * RD, RD)

    def f1(b):
        v = b % 2

        @pl.when(b >= 1)
        def _():
            rs(v, 3).wait_send()
            rs(v, 4).wait_send()

        for i in range(3):
            rs(v, i).wait_recv()
            keep[i] = keep[i] + recv0[v, i].astype(F32)
            s1[0, i] = keep[i, half(q_d, 0), :].astype(BF16)
            s1[1, i] = keep[i, half(q_d, 1), :].astype(BF16)
        rs(v, 3).start()
        rs(v, 4).start()

    def f2(b):
        v = b % 2
        rs(v, 3).wait_recv()
        rs(v, 4).wait_recv()

        @pl.when(b >= 1)
        def _():
            rs(v, 5).wait_send()
            rs(v, 6).wait_send()

        for i in range(3):
            s2[0, i, LO, :] = keep[i, half(q_x, 0), :].astype(BF16)
            s2[0, i, HI, :] = (keep[i, half(q_x, 1), :] + r1[v, 1, i].astype(F32)).astype(BF16)
            s2[1, i, LO, :] = (keep[i, half(q_y, 0), :] + r1[v, 0, i].astype(F32)).astype(BF16)
            s2[1, i, HI, :] = keep[i, half(q_y, 1), :].astype(BF16)
        rs(v, 5).start()
        rs(v, 6).start()
        for i in range(3):
            mine[i] = keep[i, block(q_me), :]

    def out_copy(b):
        return pltpu.make_async_copy(outb, out.at[(b + NC) % K], out_sem)

    def f3(b):
        v = b % 2

        @pl.when(b >= 1)
        def _():
            out_copy(b - 1).wait()

        rs(v, 5).wait_recv()
        rs(v, 6).wait_recv()
        for i in range(3):
            outb[i] = (mine[i] + r2[v, 0, i].astype(F32) + r2[v, 1, i].astype(F32)).astype(BF16)
        out_copy(b).start()

    def some(i, n):
        return pl.ds(i * n, n) if isinstance(i, int) else pl.ds(pl.multiple_of(i * n, n), n)

    def norm_tile(i):
        rows = some(i, TE)
        wide = xh[rows, :].astype(F32)
        scale = lax.rsqrt(jnp.mean(wide * wide, -1, keepdims=True) + 1e-6)
        a = (wide * scale).astype(BF16)
        a_ref[rows, :] = a
        across = a.T
        for j in range(N):
            place = ((j % 2 + core) % 2) * (N // 2) + j // 2
            at_ref[pl.ds(place * RD, RD), rows] = across[j * RD : (j + 1) * RD, :]
        acc[rows, :] = jnp.zeros((TE, D), F32)

    def norm_back(i, to):
        rows = some(i, TE)
        wide = xh[rows, :].astype(F32)
        scale = lax.rsqrt(jnp.mean(wide * wide, -1, keepdims=True) + 1e-6)
        da = acc[rows, :].astype(BF16).astype(F32)
        inner = jnp.mean(da * wide, -1, keepdims=True)
        back = (scale * da - wide * (scale * scale * scale * inner)).astype(BF16)
        to[rows, :] = (dh[rows, :].astype(F32) + back.astype(F32)).astype(BF16)

    barrier = pltpu.get_barrier_semaphore()
    for dev in (xn, yn, cn):
        pl.semaphore_signal(barrier, inc=1, device_id={"dp": dev}, device_id_type=pl.DeviceIdType.MESH)
    x_copy = pltpu.make_async_copy(x_hbm, xh, io_sem.at[0])
    dy_copy = pltpu.make_async_copy(dy_hbm, dh, io_sem.at[1])
    x_copy.start()
    dy_copy.start()
    pl.semaphore_wait(barrier, 3)
    begin(0)
    begin(1)
    x_copy.wait()
    loop(T // TE, norm_tile)
    at_out = pltpu.make_async_copy(at_ref, saved_at, io_sem.at[3])
    at_out.start()
    forward_on(0)
    begin(2)

    NT = T // TT

    def silu(both):
        gate, up = both[:, :HC], both[:, HC:]
        sig = jax.nn.sigmoid(gate)
        act = gate * sig
        return act, sig + act * (1.0 - sig), up

    def put_p(p, rows):
        across = p.T
        for j in range(N):
            place = ((j % 2 + core) % 2) * (N // 2) + j // 2
            pt[pl.ds(place * SEG, SEG), rows] = across[j * SEG : (j + 1) * SEG, :]

    def saving(g):
        return pltpu.make_async_copy(gs.at[g % 2], saved.at[g], gs_sem.at[g % 2])

    def reading(g):
        return pltpu.make_async_copy(saved.at[g], gs.at[g % 2], gs_sem.at[g % 2])

    def keep_p(c):
        return pltpu.make_async_copy(pt, saved_p.at[c], pt_sem)

    def first(c):
        slot = c % 2

        @pl.when(c + 1 < NC)
        def _():
            forward_on(c + 1)

        @pl.when(c + 3 < NC)
        def _():
            begin(c + 3)

        @pl.when(c == NC - 2)
        def _():
            begin(NC)

        @pl.when(c < NC - 1)
        def _():
            finish(c)
            load(c)

        load_wait(c)

        def tile(i):
            @pl.when((c == NC - 2) & (i == NT - 2))
            def _():
                finish(NC - 1)
                load(NC - 1)

            @pl.when((c == NC - 1) & (i == 1))
            def _():
                forward_on(NC)
                begin(NC + 1)
                begin(NC + 2)

            g = c * NT + i

            @pl.when(g >= 2)
            def _():
                saving(g - 2).wait()

            @pl.when((c >= 1) & (i == 0))
            def _():
                keep_p(c - 1).wait()

            rows = some(i, TT)
            both = dot(a_ref[rows, :], wgu[slot])
            act, slope, up = silu(both)
            gs[g % 2, :, pl.ds(0, HC)] = act
            gs[g % 2, :, pl.ds(HC, HC)] = slope * up
            saving(g).start()
            p = (act * up).astype(BF16)
            put_p(p, rows)
            acc[rows, :] = acc[rows, :] + dot(p, wdn[slot])

        loop(NT, tile)
        keep_p(c).start()

    loop(NC, first)

    def next_state(i):
        @pl.when(i == T // TE - 3)
        def _():
            finish(NC)
            load(NC)

        rows = some(i, TE)
        xh[rows, :] = (xh[rows, :].astype(F32) + acc[rows, :].astype(BF16).astype(F32)).astype(BF16)
        norm_tile(i)

    at_out.wait()
    loop(T // TE, next_state)
    dy_copy.wait()
    keep_p(NC - 1).wait()
    saving(NC * NT - 2).wait()
    saving(NC * NT - 1).wait()
    reading(0).start()
    reading(1).start()

    def get_p(c):
        return pltpu.make_async_copy(saved_p.at[c], pt, pt_sem)

    at_in = pltpu.make_async_copy(saved_at, at_ref, io_sem.at[3])

    def add_da(s, buf):
        slot = (s + NC) % 2
        for i in range(NT):
            rows = some(i, TT)
            acc[rows, :] = acc[rows, :] + dot_nt(buf[rows, :], wgu[slot])

    def backward(s, n, tile, buf, da=None):
        load_wait(s + NC)
        slot = (s + NC) % 2
        v = s % 2

        @pl.when((s >= 1) & (s + NC + 1 < K))
        def _():
            forward_on(s + NC + 1)

        loop(n, lambda i: tile(s, i, slot, buf))

        @pl.when(s >= 2)
        def _():
            f3(s - 2)

        @pl.when(s >= 1)
        def _():
            f2(s - 1)
            for m in range(3):
                rs(v, m).wait_send()

        @pl.when(s == 0)
        def _():
            forward_on(NC + 1)

        @pl.when(s + NC + 3 < K)
        def _():
            begin(s + NC + 3)

        @pl.when(s >= NC)
        def _():
            get_p(s - NC).wait()

        top, low = pl.ds(0, D // 2), pl.ds(D // 2, D // 2)
        both = dot(at_ref[low, :], buf[...])
        for i in range(2):
            send0[i] = both[:, i * HC : (i + 1) * HC].astype(BF16)
            rs(v, i).start()
        down = dot(pt[pl.ds(HC // 2, HC // 2), :], dh[...])
        for q in range(N // 2):
            for h in range(2):
                to = pl.ds(q * RD + h * SEG, SEG)
                send0[2, to, :] = down[q * SEG : (q + 1) * SEG, h * HC : (h + 1) * HC].astype(BF16)
        rs(v, 2).start()
        both = dot(at_ref[top, :], buf[...])
        for i in range(2):
            keep[i] = both[:, i * HC : (i + 1) * HC]
        down = dot(pt[pl.ds(0, HC // 2), :], dh[...])
        for q in range(N // 2):
            for h in range(2):
                to = pl.ds(q * RD + h * SEG, SEG)
                keep[2, to, :] = down[q * SEG : (q + 1) * SEG, h * HC : (h + 1) * HC]

        @pl.when((s >= NC - 1) & (s + 1 < K))
        def _():
            get_p(s + 1 - NC).start()

        @pl.when(s == NC - 1)
        def _():
            at_in.start()

        f1(s)

        @pl.when(s + NC + 1 < K)
        def _():
            finish(s + NC + 1)

        @pl.when(s + 1 < K)
        def _():
            load(s + NC + 1)

        if da is not None:
            pl.when(da(s))(lambda: add_da(s, buf))

    def back_to(rows, act, slope, slot, buf):
        dp = dot_nt(dh[rows, :], wdn[slot]).astype(BF16).astype(F32)
        buf[rows, pl.ds(HC, HC)] = (dp * act).astype(BF16)
        buf[rows, pl.ds(0, HC)] = (dp * slope).astype(BF16)

    def computed(s, i, slot, buf):
        rows = some(i, TB)
        act, slope, up = silu(dot(a_ref[rows, :], wgu[slot]))
        back_to(rows, act, slope * up, slot, buf)
        put_p((act * up).astype(BF16), rows)

    def read_back(s, i, slot, buf):
        g = (s - NC) * NT + i
        reading(g).wait()
        back_to(some(i, TT), gs[g % 2, :, pl.ds(0, HC)], gs[g % 2, :, pl.ds(HC, HC)], slot, buf)

        @pl.when(g + 2 < NC * NT)
        def _():
            reading(g + 2).start()

    loop(NC, lambda s: backward(s, T // TB, computed, dgu, lambda s: s >= 0))

    def change(i):
        norm_back(i, dh)
        rows = some(i, TE)
        acc[rows, :] = jnp.zeros((TE, D), F32)

    loop(T // TE, change)
    x_again = pltpu.make_async_copy(x_hbm, xh, io_sem.at[0])
    x_again.start()
    at_in.wait()

    def last_layer(s):
        backward(s, NT, read_back, two.at[1 - s // (K - 1)], lambda s: s < K - 2)

    loop(NC, lambda s: last_layer(s + NC))

    def late_da(j):
        @pl.when(j == 1)
        def _():
            x_again.wait()
            f3(K - 2)
            f2(K - 1)

        add_da(K - 2 + j, two.at[1 - j])

    loop(2, late_da)
    loop(T // TE, lambda i: norm_back(i, a_ref))
    dx_copy = pltpu.make_async_copy(a_ref, dx_hbm, io_sem.at[1])
    dx_copy.start()
    f3(K - 1)
    out_copy(K - 1).wait()
    dx_copy.wait()
    for m in range(7):
        rs(1, m).wait_send()

    def drain(k):
        for m in range(8):
            ag(k, m).wait_send()

    loop(K, drain)


def mlp_stack(x, dy, own):
    any_space = pl.BlockSpec(memory_space=pl.ANY)
    vm = pltpu.VMEM
    flops = 17 * 2 * T * D * FF
    return pl.pallas_call(
        kernel,
        name="mlp_stack",
        out_shape=[
            jax.ShapeDtypeStruct((T, D), BF16),
            jax.ShapeDtypeStruct((K, 3, RD, HC), BF16),
            jax.ShapeDtypeStruct((K, N, 3, RD, HC), BF16),
            jax.ShapeDtypeStruct((NC * (T // TT), TT, 2 * HC), F32),
            jax.ShapeDtypeStruct((NC, HC, T), BF16),
            jax.ShapeDtypeStruct((D, T), BF16),
        ],
        in_specs=[any_space] * 3,
        out_specs=[any_space] * 6,
        scratch_shapes=[
            vm((T, D), BF16), vm((2, T, D), BF16), vm((D, T), BF16), vm((T, D), BF16), vm((T, D), F32),
            vm((2, D, 2 * HC), BF16), vm((2, HC, D), BF16),
            vm((HC, T), BF16), vm((2, TT, 2 * HC), F32),
            vm((3, D // 2, HC), F32), vm((3, RD, HC), F32), vm((3, D // 2, HC), BF16), vm((2, 3, D // 2, HC), BF16),
            vm((2, 3, RD // 2, HC), BF16), vm((2, 2, 3, RD // 2, HC), BF16),
            vm((2, 3, RD, HC), BF16), vm((2, 2, 3, RD, HC), BF16), vm((3, RD, HC), BF16),
            pltpu.SemaphoreType.DMA((K, 8)), pltpu.SemaphoreType.DMA((K, 8)),
            pltpu.SemaphoreType.DMA((7,)), pltpu.SemaphoreType.DMA((2, 7)),
            pltpu.SemaphoreType.DMA((2,)), pltpu.SemaphoreType.DMA((2,)),
            pltpu.SemaphoreType.DMA((4,)), pltpu.SemaphoreType.DMA, pltpu.SemaphoreType.DMA((2,)), pltpu.SemaphoreType.DMA,
        ],
        compiler_params=pltpu.CompilerParams(
            collective_id=0, has_side_effects=True, vmem_limit_bytes=67_000_000
        ),
        cost_estimate=pl.CostEstimate(flops=flops, bytes_accessed=10**8, transcendentals=T * FF),
    )(x, dy, own)


def cut_kernel(wg, wu, wd, own):
    for c in range(NC):
        for i, w in enumerate((wg, wu)):
            parts = [w[0, :, j * (FF // N) + c * SEG : j * (FF // N) + (c + 1) * SEG] for j in range(N)]
            own[c, i] = jnp.concatenate(parts, axis=1)
        for h in range(2):
            own[c, 2, h * SEG : (h + 1) * SEG, :] = wd[0, c * SEG : (c + 1) * SEG, h * HC : (h + 1) * HC]


def cut(wg, wu, wd):
    return pl.pallas_call(
        cut_kernel,
        name="cut",
        grid=(L,),
        out_shape=jax.ShapeDtypeStruct((K, 3, RD, HC), BF16),
        in_specs=[
            pl.BlockSpec((1, RD, FF), lambda n: (n, 0, 0)),
            pl.BlockSpec((1, RD, FF), lambda n: (n, 0, 0)),
            pl.BlockSpec((1, FF // N, D), lambda n: (n, 0, 0)),
        ],
        out_specs=pl.BlockSpec((NC, 3, RD, HC), lambda n: (n, 0, 0, 0)),
    )(wg, wu, wd)


def join_kernel(dx_in, got, dx, wg, wu, wd):
    dx[...] = dx_in[...]
    for i, w in enumerate((wg, wu)):
        parts = [got[c, i, :, j * SEG : (j + 1) * SEG] for j in range(N) for c in range(NC)]
        w[0] = jnp.concatenate(parts, axis=1)
    for c in range(NC):
        for h in range(2):
            wd[0, c * SEG : (c + 1) * SEG, h * HC : (h + 1) * HC] = got[c, 2, h * SEG : (h + 1) * SEG, :]


def join(dx, got):
    return pl.pallas_call(
        join_kernel,
        name="join",
        grid=(L,),
        out_shape=[
            jax.ShapeDtypeStruct((T, D), BF16),
            jax.ShapeDtypeStruct((L, RD, FF), BF16),
            jax.ShapeDtypeStruct((L, RD, FF), BF16),
            jax.ShapeDtypeStruct((L, FF // N, D), BF16),
        ],
        in_specs=[
            pl.BlockSpec((T // L, D), lambda n: (n, 0)),
            pl.BlockSpec((NC, 3, RD, HC), lambda n: (n, 0, 0, 0)),
        ],
        out_specs=[
            pl.BlockSpec((T // L, D), lambda n: (n, 0)),
            pl.BlockSpec((1, RD, FF), lambda n: (n, 0, 0)),
            pl.BlockSpec((1, RD, FF), lambda n: (n, 0, 0)),
            pl.BlockSpec((1, FF // N, D), lambda n: (n, 0, 0)),
        ],
    )(dx, got)


def solution(mesh):
    def body(x, dy, wg, wu, wd):
        dx, got, *_ = mlp_stack(x[0], dy[0], cut(wg, wu, wd))
        dx, by_g, by_u, by_d = join(dx, got)
        return dx[None], by_g, by_u, by_d

    act = P(("rep", "dp"), None, None)
    w = P(None, "dp", None)
    return jax.shard_map(
        body, mesh=mesh, in_specs=(act, act, w, w, w), out_specs=(act, *[P("rep", "dp", None)] * 3), check_vma=False
    )
```

```python
import jax
import jax.numpy as jnp
from jax import lax
from jax.experimental import pallas as pl
from jax.experimental.pallas import tpu as pltpu
from jax.sharding import PartitionSpec as P

F32, BF16 = jnp.float32, jnp.bfloat16
T, D, FF, L, N = 2048, 1024, 2560, 2, 8
NC = 5
HC = FF // NC
SEG = HC // N
RD = D // N
K = L * NC
TT = 512
TB = 1024
TE = 256
NN = (((1,), (0,)), ((), ()))
NT_DIMS = (((1,), (1,)), ((), ()))


def dot(a, b):
    return lax.dot_general(a, b, NN, preferred_element_type=F32)


def dot_nt(a, b):
    return lax.dot_general(a, b, NT_DIMS, preferred_element_type=F32)


def kernel(
    x_hbm, dy_hbm, own,
    dx_hbm, out, land, saved, saved_p, saved_at,
    xh, two, at_ref, dh, acc, wgu, wdn, pt, gs,
    keep, mine, send0, recv0, s1, r1, s2, r2, outb,
    ag_send, ag_recv, rs_send, rs_recv, gu_sem, wd_sem, io_sem, out_sem, gs_sem, pt_sem,
):
    a_ref, dgu = two.at[0], two.at[1]
    me = lax.axis_index("dp")
    core = me % 2
    ypos = (me // 2) % 2
    xpos = me // 4
    xn = (1 - xpos) * 4 + ypos * 2 + core
    yn = xpos * 4 + (1 - ypos) * 2 + core
    cn = xpos * 4 + ypos * 2 + (1 - core)
    diag = (1 - xpos) * 4 + (1 - ypos) * 2 + core
    q_me, q_x, q_y, q_d = me // 2, xn // 2, yn // 2, diag // 2

    def remote(src, dst, ssem, rsem, dev):
        return pltpu.make_async_remote_copy(
            src_ref=src, dst_ref=dst, send_sem=ssem, recv_sem=rsem,
            device_id={"dp": dev}, device_id_type=pl.DeviceIdType.MESH,
        )

    def loop(n, f):
        lax.fori_loop(0, n, lambda i, _: (f(i), 0)[1], 0)

    LO, HI = pl.ds(0, RD // 2), pl.ds(RD // 2, RD // 2)

    def ag(k, m, arriving=False):
        if m < 3:
            dev, src, dst, got = (xn, yn, cn)[m], own.at[k], land.at[k, me], land.at[k, (xn, yn, cn)[m]]
        elif m == 3:
            dev, src, dst, got = yn, land.at[k, xn, :, LO], land.at[k, xn, :, LO], land.at[k, diag, :, LO]
        elif m == 4:
            dev, src, dst, got = xn, land.at[k, yn, :, HI], land.at[k, yn, :, HI], land.at[k, diag, :, HI]
        else:
            b = (xn, yn, diag)[m - 5]
            there = (b // 2) * 2 + (1 - core)
            dev, src, dst, got = cn, land.at[k, b], land.at[k, b], land.at[k, there]
        if arriving:
            src = dst = got
        return remote(src, dst, ag_send.at[k, m], ag_recv.at[k, m], dev)

    def ag_start(k, ms):
        for m in ms:
            ag(k, m).start()

    def ag_wait(k, ms):
        for m in ms:
            ag(k, m, True).wait_recv()

    def load(p):
        k, slot = p % K, p % 2
        for r in range(N):
            if r == 0:
                j, src = me, own.at[k]
            else:
                fx, fy, fc = r // 4, (r // 2) % 2, r % 2
                j = ((xpos + fx) % 2) * 4 + ((ypos + fy) % 2) * 2 + (core + fc) % 2
                src = land.at[k, j]
            rows, segs = pl.ds(j * RD, RD), pl.ds(j * SEG, SEG)
            for h in range(2):
                cols = pl.ds(h * HC, HC)
                pltpu.make_async_copy(src.at[h], wgu.at[slot, rows, cols], gu_sem.at[slot]).start()
                pltpu.make_async_copy(
                    src.at[2, pl.ds(h * SEG, SEG)], wdn.at[slot, segs, cols], wd_sem.at[slot]
                ).start()

    def load_wait(p):
        slot = p % 2
        pltpu.make_async_copy(wgu.at[slot], wgu.at[slot], gu_sem.at[slot]).wait()
        pltpu.make_async_copy(wdn.at[slot], wdn.at[slot], wd_sem.at[slot]).wait()

    def begin(k):
        ag_start(k, (0, 1, 2))

    def forward_on(k):
        ag_wait(k, (0, 1))
        ag_start(k, (3, 4, 5, 6))

    def finish(k):
        ag_wait(k, (3, 4))
        ag_start(k, (7,))
        ag_wait(k, (2, 5, 6, 7))

    def rs(v, m):
        if m < 3:
            src, dst, dev = send0.at[m], recv0.at[v, m], cn
        else:
            i = (m - 3) % 2
            src, dst = (s1.at[i], r1.at[v, i]) if m < 5 else (s2.at[i], r2.at[v, i])
            dev = (xn, yn)[i]
        return remote(src, dst, rs_send.at[m], rs_recv.at[v, m], dev)

    def half(q, h):
        return pl.ds(q * RD + h * (RD // 2), RD // 2)

    def block(q):
        return pl.ds(q * RD, RD)

    def f1(b):
        v = b % 2

        @pl.when(b >= 1)
        def _():
            rs(v, 3).wait_send()
            rs(v, 4).wait_send()

        for i in range(3):
            rs(v, i).wait_recv()
            keep[i] = keep[i] + recv0[v, i].astype(F32)
            s1[0, i] = keep[i, half(q_d, 0), :].astype(BF16)
            s1[1, i] = keep[i, half(q_d, 1), :].astype(BF16)
        rs(v, 3).start()
        rs(v, 4).start()

    def f2(b):
        v = b % 2
        rs(v, 3).wait_recv()
        rs(v, 4).wait_recv()

        @pl.when(b >= 1)
        def _():
            rs(v, 5).wait_send()
            rs(v, 6).wait_send()

        for i in range(3):
            s2[0, i, LO, :] = keep[i, half(q_x, 0), :].astype(BF16)
            s2[0, i, HI, :] = (keep[i, half(q_x, 1), :] + r1[v, 1, i].astype(F32)).astype(BF16)
            s2[1, i, LO, :] = (keep[i, half(q_y, 0), :] + r1[v, 0, i].astype(F32)).astype(BF16)
            s2[1, i, HI, :] = keep[i, half(q_y, 1), :].astype(BF16)
        rs(v, 5).start()
        rs(v, 6).start()
        for i in range(3):
            mine[i] = keep[i, block(q_me), :]

    def out_copy(b):
        return pltpu.make_async_copy(outb, out.at[(b + NC) % K], out_sem)

    def f3(b):
        v = b % 2

        @pl.when(b >= 1)
        def _():
            out_copy(b - 1).wait()

        rs(v, 5).wait_recv()
        rs(v, 6).wait_recv()
        for i in range(3):
            outb[i] = (mine[i] + r2[v, 0, i].astype(F32) + r2[v, 1, i].astype(F32)).astype(BF16)
        out_copy(b).start()

    def some(i, n):
        return pl.ds(i * n, n) if isinstance(i, int) else pl.ds(pl.multiple_of(i * n, n), n)

    def norm_tile(i):
        rows = some(i, TE)
        wide = xh[rows, :].astype(F32)
        scale = lax.rsqrt(jnp.mean(wide * wide, -1, keepdims=True) + 1e-6)
        a = (wide * scale).astype(BF16)
        a_ref[rows, :] = a
        across = a.T
        for j in range(N):
            place = ((j % 2 + core) % 2) * (N // 2) + j // 2
            at_ref[pl.ds(place * RD, RD), rows] = across[j * RD : (j + 1) * RD, :]
        acc[rows, :] = jnp.zeros((TE, D), F32)

    def norm_back(i, to):
        rows = some(i, TE)
        wide = xh[rows, :].astype(F32)
        scale = lax.rsqrt(jnp.mean(wide * wide, -1, keepdims=True) + 1e-6)
        da = acc[rows, :].astype(BF16).astype(F32)
        inner = jnp.mean(da * wide, -1, keepdims=True)
        back = (scale * da - wide * (scale * scale * scale * inner)).astype(BF16)
        to[rows, :] = (dh[rows, :].astype(F32) + back.astype(F32)).astype(BF16)

    barrier = pltpu.get_barrier_semaphore()
    for dev in (xn, yn, cn):
        pl.semaphore_signal(barrier, inc=1, device_id={"dp": dev}, device_id_type=pl.DeviceIdType.MESH)
    x_copy = pltpu.make_async_copy(x_hbm, xh, io_sem.at[0])
    dy_copy = pltpu.make_async_copy(dy_hbm, dh, io_sem.at[1])
    x_copy.start()
    dy_copy.start()
    pl.semaphore_wait(barrier, 3)
    begin(0)
    begin(1)
    x_copy.wait()
    loop(T // TE, norm_tile)
    at_out = pltpu.make_async_copy(at_ref, saved_at, io_sem.at[3])
    at_out.start()
    forward_on(0)
    begin(2)

    NT = T // TT

    def silu(both):
        gate, up = both[:, :HC], both[:, HC:]
        sig = jax.nn.sigmoid(gate)
        act = gate * sig
        return act, sig + act * (1.0 - sig), up

    def put_p(p, rows):
        across = p.T
        for j in range(N):
            place = ((j % 2 + core) % 2) * (N // 2) + j // 2
            pt[pl.ds(place * SEG, SEG), rows] = across[j * SEG : (j + 1) * SEG, :]

    def saving(g):
        return pltpu.make_async_copy(gs.at[g % 2], saved.at[g], gs_sem.at[g % 2])

    def reading(g):
        return pltpu.make_async_copy(saved.at[g], gs.at[g % 2], gs_sem.at[g % 2])

    def keep_p(c):
        return pltpu.make_async_copy(pt, saved_p.at[c], pt_sem)

    def first(c):
        slot = c % 2

        @pl.when(c + 1 < NC)
        def _():
            forward_on(c + 1)

        @pl.when(c + 3 < NC)
        def _():
            begin(c + 3)

        @pl.when(c == NC - 2)
        def _():
            begin(NC)

        @pl.when(c < NC - 1)
        def _():
            finish(c)
            load(c)

        load_wait(c)

        def tile(i):
            @pl.when((c == NC - 2) & (i == NT - 2))
            def _():
                finish(NC - 1)
                load(NC - 1)

            @pl.when((c == NC - 1) & (i == 1))
            def _():
                forward_on(NC)
                begin(NC + 1)
                begin(NC + 2)

            g = c * NT + i

            @pl.when(g >= 2)
            def _():
                saving(g - 2).wait()

            @pl.when((c >= 1) & (i == 0))
            def _():
                keep_p(c - 1).wait()

            rows = some(i, TT)
            both = dot(a_ref[rows, :], wgu[slot])
            act, slope, up = silu(both)
            gs[g % 2, :, pl.ds(0, HC)] = act
            gs[g % 2, :, pl.ds(HC, HC)] = slope * up
            saving(g).start()
            p = (act * up).astype(BF16)
            put_p(p, rows)
            acc[rows, :] = acc[rows, :] + dot(p, wdn[slot])

        loop(NT, tile)
        keep_p(c).start()

    loop(NC, first)

    def next_state(i):
        @pl.when(i == T // TE - 3)
        def _():
            finish(NC)
            load(NC)

        rows = some(i, TE)
        xh[rows, :] = (xh[rows, :].astype(F32) + acc[rows, :].astype(BF16).astype(F32)).astype(BF16)
        norm_tile(i)

    at_out.wait()
    loop(T // TE, next_state)
    dy_copy.wait()
    keep_p(NC - 1).wait()
    saving(NC * NT - 2).wait()
    saving(NC * NT - 1).wait()
    reading(0).start()
    reading(1).start()

    def get_p(c):
        return pltpu.make_async_copy(saved_p.at[c], pt, pt_sem)

    at_in = pltpu.make_async_copy(saved_at, at_ref, io_sem.at[3])

    def add_da(s, buf):
        slot = (s + NC) % 2
        for i in range(NT):
            rows = some(i, TT)
            acc[rows, :] = acc[rows, :] + dot_nt(buf[rows, :], wgu[slot])

    def backward(s, n, tile, buf, da=None):
        load_wait(s + NC)
        slot = (s + NC) % 2
        v = s % 2

        @pl.when((s >= 1) & (s + NC + 1 < K))
        def _():
            forward_on(s + NC + 1)

        loop(n, lambda i: tile(s, i, slot, buf))

        @pl.when(s >= 2)
        def _():
            f3(s - 2)

        @pl.when(s >= 1)
        def _():
            f2(s - 1)
            for m in range(3):
                rs(v, m).wait_send()

        @pl.when(s == 0)
        def _():
            forward_on(NC + 1)

        @pl.when(s >= NC)
        def _():
            get_p(s - NC).wait()

        top, low = pl.ds(0, D // 2), pl.ds(D // 2, D // 2)
        both = dot(at_ref[low, :], buf[...])
        for i in range(2):
            send0[i] = both[:, i * HC : (i + 1) * HC].astype(BF16)
            rs(v, i).start()
        down = dot(pt[pl.ds(HC // 2, HC // 2), :], dh[...])
        for q in range(N // 2):
            for h in range(2):
                to = pl.ds(q * RD + h * SEG, SEG)
                send0[2, to, :] = down[q * SEG : (q + 1) * SEG, h * HC : (h + 1) * HC].astype(BF16)
        rs(v, 2).start()
        both = dot(at_ref[top, :], buf[...])
        for i in range(2):
            keep[i] = both[:, i * HC : (i + 1) * HC]
        down = dot(pt[pl.ds(0, HC // 2), :], dh[...])
        for q in range(N // 2):
            for h in range(2):
                to = pl.ds(q * RD + h * SEG, SEG)
                keep[2, to, :] = down[q * SEG : (q + 1) * SEG, h * HC : (h + 1) * HC]

        @pl.when((s >= NC - 1) & (s + 1 < K))
        def _():
            get_p(s + 1 - NC).start()

        @pl.when(s == NC - 1)
        def _():
            at_in.start()

        f1(s)

        @pl.when(s + NC + 3 < K)
        def _():
            begin(s + NC + 3)

        @pl.when(s + NC + 1 < K)
        def _():
            finish(s + NC + 1)

        @pl.when(s + 1 < K)
        def _():
            load(s + NC + 1)

        if da is not None:
            pl.when(da(s))(lambda: add_da(s, buf))

    def back_to(rows, act, slope, slot, buf):
        dp = dot_nt(dh[rows, :], wdn[slot]).astype(BF16).astype(F32)
        buf[rows, pl.ds(HC, HC)] = (dp * act).astype(BF16)
        buf[rows, pl.ds(0, HC)] = (dp * slope).astype(BF16)

    def computed(s, i, slot, buf):
        rows = some(i, TB)
        act, slope, up = silu(dot(a_ref[rows, :], wgu[slot]))
        back_to(rows, act, slope * up, slot, buf)
        put_p((act * up).astype(BF16), rows)

    def read_back(s, i, slot, buf):
        g = (s - NC) * NT + i
        reading(g).wait()
        back_to(some(i, TT), gs[g % 2, :, pl.ds(0, HC)], gs[g % 2, :, pl.ds(HC, HC)], slot, buf)

        @pl.when(g + 2 < NC * NT)
        def _():
            reading(g + 2).start()

    loop(NC, lambda s: backward(s, T // TB, computed, dgu, lambda s: s >= 0))

    def change(i):
        norm_back(i, dh)
        rows = some(i, TE)
        acc[rows, :] = jnp.zeros((TE, D), F32)

    loop(T // TE, change)
    x_again = pltpu.make_async_copy(x_hbm, xh, io_sem.at[0])
    x_again.start()
    at_in.wait()

    def last_layer(s):
        backward(s, NT, read_back, two.at[1 - s // (K - 1)], lambda s: s < K - 2)

    loop(NC, lambda s: last_layer(s + NC))

    def late_da(j):
        @pl.when(j == 1)
        def _():
            x_again.wait()
            f3(K - 2)
            f2(K - 1)

        add_da(K - 2 + j, two.at[1 - j])

    loop(2, late_da)
    loop(T // TE, lambda i: norm_back(i, a_ref))
    dx_copy = pltpu.make_async_copy(a_ref, dx_hbm, io_sem.at[1])
    dx_copy.start()
    f3(K - 1)
    out_copy(K - 1).wait()
    dx_copy.wait()
    for m in range(7):
        rs(1, m).wait_send()

    def drain(k):
        for m in range(8):
            ag(k, m).wait_send()

    loop(K, drain)


def mlp_stack(x, dy, own):
    any_space = pl.BlockSpec(memory_space=pl.ANY)
    vm = pltpu.VMEM
    flops = 17 * 2 * T * D * FF
    return pl.pallas_call(
        kernel,
        name="mlp_stack",
        out_shape=[
            jax.ShapeDtypeStruct((T, D), BF16),
            jax.ShapeDtypeStruct((K, 3, RD, HC), BF16),
            jax.ShapeDtypeStruct((K, N, 3, RD, HC), BF16),
            jax.ShapeDtypeStruct((NC * (T // TT), TT, 2 * HC), F32),
            jax.ShapeDtypeStruct((NC, HC, T), BF16),
            jax.ShapeDtypeStruct((D, T), BF16),
        ],
        in_specs=[any_space] * 3,
        out_specs=[any_space] * 6,
        scratch_shapes=[
            vm((T, D), BF16), vm((2, T, D), BF16), vm((D, T), BF16), vm((T, D), BF16), vm((T, D), F32),
            vm((2, D, 2 * HC), BF16), vm((2, HC, D), BF16),
            vm((HC, T), BF16), vm((2, TT, 2 * HC), F32),
            vm((3, D // 2, HC), F32), vm((3, RD, HC), F32), vm((3, D // 2, HC), BF16), vm((2, 3, D // 2, HC), BF16),
            vm((2, 3, RD // 2, HC), BF16), vm((2, 2, 3, RD // 2, HC), BF16),
            vm((2, 3, RD, HC), BF16), vm((2, 2, 3, RD, HC), BF16), vm((3, RD, HC), BF16),
            pltpu.SemaphoreType.DMA((K, 8)), pltpu.SemaphoreType.DMA((K, 8)),
            pltpu.SemaphoreType.DMA((7,)), pltpu.SemaphoreType.DMA((2, 7)),
            pltpu.SemaphoreType.DMA((2,)), pltpu.SemaphoreType.DMA((2,)),
            pltpu.SemaphoreType.DMA((4,)), pltpu.SemaphoreType.DMA, pltpu.SemaphoreType.DMA((2,)), pltpu.SemaphoreType.DMA,
        ],
        compiler_params=pltpu.CompilerParams(
            collective_id=0, has_side_effects=True, vmem_limit_bytes=67_000_000
        ),
        cost_estimate=pl.CostEstimate(flops=flops, bytes_accessed=10**8, transcendentals=T * FF),
    )(x, dy, own)


def cut_kernel(wg, wu, wd, own):
    for c in range(NC):
        for i, w in enumerate((wg, wu)):
            parts = [w[0, :, j * (FF // N) + c * SEG : j * (FF // N) + (c + 1) * SEG] for j in range(N)]
            own[c, i] = jnp.concatenate(parts, axis=1)
        for h in range(2):
            own[c, 2, h * SEG : (h + 1) * SEG, :] = wd[0, c * SEG : (c + 1) * SEG, h * HC : (h + 1) * HC]


def cut(wg, wu, wd):
    return pl.pallas_call(
        cut_kernel,
        name="cut",
        grid=(L,),
        out_shape=jax.ShapeDtypeStruct((K, 3, RD, HC), BF16),
        in_specs=[
            pl.BlockSpec((1, RD, FF), lambda n: (n, 0, 0)),
            pl.BlockSpec((1, RD, FF), lambda n: (n, 0, 0)),
            pl.BlockSpec((1, FF // N, D), lambda n: (n, 0, 0)),
        ],
        out_specs=pl.BlockSpec((NC, 3, RD, HC), lambda n: (n, 0, 0, 0)),
    )(wg, wu, wd)


def join_kernel(dx_in, got, dx, wg, wu, wd):
    dx[...] = dx_in[...]
    for i, w in enumerate((wg, wu)):
        parts = [got[c, i, :, j * SEG : (j + 1) * SEG] for j in range(N) for c in range(NC)]
        w[0] = jnp.concatenate(parts, axis=1)
    for c in range(NC):
        for h in range(2):
            wd[0, c * SEG : (c + 1) * SEG, h * HC : (h + 1) * HC] = got[c, 2, h * SEG : (h + 1) * SEG, :]


def join(dx, got):
    return pl.pallas_call(
        join_kernel,
        name="join",
        grid=(L,),
        out_shape=[
            jax.ShapeDtypeStruct((T, D), BF16),
            jax.ShapeDtypeStruct((L, RD, FF), BF16),
            jax.ShapeDtypeStruct((L, RD, FF), BF16),
            jax.ShapeDtypeStruct((L, FF // N, D), BF16),
        ],
        in_specs=[
            pl.BlockSpec((T // L, D), lambda n: (n, 0)),
            pl.BlockSpec((NC, 3, RD, HC), lambda n: (n, 0, 0, 0)),
        ],
        out_specs=[
            pl.BlockSpec((T // L, D), lambda n: (n, 0)),
            pl.BlockSpec((1, RD, FF), lambda n: (n, 0, 0)),
            pl.BlockSpec((1, RD, FF), lambda n: (n, 0, 0)),
            pl.BlockSpec((1, FF // N, D), lambda n: (n, 0, 0)),
        ],
    )(dx, got)


def solution(mesh):
    def body(x, dy, wg, wu, wd):
        dx, got, *_ = mlp_stack(x[0], dy[0], cut(wg, wu, wd))
        dx, by_g, by_u, by_d = join(dx, got)
        return dx[None], by_g, by_u, by_d

    act = P(("rep", "dp"), None, None)
    w = P(None, "dp", None)
    return jax.shard_map(
        body, mesh=mesh, in_specs=(act, act, w, w, w), out_specs=(act, *[P("rep", "dp", None)] * 3), check_vma=False
    )
```
